8 devices in a mesh: dp: 2 (over z, y), ep: 4 (over x, core).
Axes of the slice: x: 2, y: 2, z: 1, core: 2. Of those that a mesh axis runs over, the one named last changes fastest.
Arguments:
- x_a: bfloat16 [2048, 2048], P(('dp', 'ep')), parts along dimension 0
- route_a: int32 [2048, 4], P(('dp', 'ep')), parts along dimension 0
- gate_a: float32 [2048, 4], P(('dp', 'ep')), parts along dimension 0
- h_b: bfloat16 [2048, 2048], P(('dp', 'ep')), parts along dimension 0
- attn_b: bfloat16 [2048, 2048], P(('dp', 'ep')), parts along dimension 0
- route_b: int32 [2048, 4], P(('dp', 'ep')), parts along dimension 0
- gate_b: float32 [2048, 4], P(('dp', 'ep')), parts along dimension 0
- w_qkv: bfloat16 [2048, 6144], replicated
- w_o: bfloat16 [2048, 2048], replicated
- w_gate: bfloat16 [60, 2048, 1408], P('ep')
- w_up: bfloat16 [60, 2048, 1408], P('ep')
- w_down: bfloat16 [60, 1408, 2048], P('ep')
Outputs:
- output 1: bfloat16 [2048, 2048], P(('dp', 'ep')), parts along dimension 0
- output 2: bfloat16 [2048, 2048], P(('dp', 'ep')), parts along dimension 0
- output 3: bfloat16 [2048, 6144], P(('dp', 'ep')), parts along dimension 0
There are 2 independent parts. The reference program is written for one: setup_inputs(seed, part) draws one part's arguments, and reference() takes and returns one part's arrays. A program takes and returns all parts, laid end to end along the dimension named above; an argument that names none is the same for every part.
All inputs are finite; a program needn't handle non-finite values.
Results may differ from the reference program's by a relative error of at most 0.0114635.
Values are sent between devices in bfloat16 or wider.
A program may use at most 1.25 GiB of HBM per device.

```python
import jax
import jax.numpy as jnp
from jax import lax

MODEL_DIM = 2048
FF_DIM = 1408
NUM_EXPERTS = 60
TOP_K = 4
NUM_HEADS = 16
KV_HEADS = 16
HEAD_DIM = 128
TOKENS_DEV = 256
GROUP_DEVS = 4

CAPACITY = min(TOKENS_DEV, 2 * ((TOKENS_DEV * TOP_K + NUM_EXPERTS - 1) // NUM_EXPERTS))
LOCAL_EXPERTS = NUM_EXPERTS // GROUP_DEVS
QKV_DIM = (NUM_HEADS + 2 * KV_HEADS) * HEAD_DIM
ATTN_DIM = NUM_HEADS * HEAD_DIM
GROUP_ROWS = GROUP_DEVS * TOKENS_DEV
HOT_DEVS = max(1, GROUP_DEVS // 4)


def source_routing(rng_key, dev_order):
    key_local, key_want, key_rows = jax.random.split(rng_key, 3)
    local_order = jax.vmap(lambda sub_key: jax.random.permutation(sub_key, LOCAL_EXPERTS))(jax.random.split(key_local, GROUP_DEVS))
    visits = jnp.arange(NUM_EXPERTS)
    visit_dev = dev_order[visits % GROUP_DEVS]
    visit_expert = visit_dev * LOCAL_EXPERTS + local_order[visit_dev, visits // GROUP_DEVS]
    wanted = jax.random.randint(key_want, (NUM_EXPERTS,), 1, CAPACITY + 1)
    wanted = jnp.where(visits % GROUP_DEVS < HOT_DEVS, CAPACITY, wanted)
    wanted = jnp.where(visits < GROUP_DEVS, 1, wanted)
    wanted = jnp.where(visits == 0, CAPACITY, wanted)
    n_entries = TOKENS_DEV * TOP_K
    first_pass = jnp.clip(n_entries - (jnp.cumsum(wanted) - wanted), 0, wanted)
    room_left = CAPACITY - first_pass
    left_over = n_entries - jnp.sum(first_pass)
    second_pass = jnp.clip(left_over - (jnp.cumsum(room_left) - room_left), 0, room_left)
    run_ends = jnp.cumsum(first_pass + second_pass)
    positions = jnp.arange(n_entries)
    run_index = jnp.sum((run_ends[None, :] <= positions[:, None]).astype(jnp.int32), axis=1)
    choices = visit_expert[run_index].reshape(TOP_K, TOKENS_DEV).T
    return choices[jax.random.permutation(key_rows, TOKENS_DEV)]


def group_routing(rng_key):
    key_order, key_src = jax.random.split(rng_key)
    dev_order = jax.random.permutation(key_order, GROUP_DEVS)
    per_source = jax.vmap(lambda sub_key: source_routing(sub_key, dev_order))(jax.random.split(key_src, GROUP_DEVS))
    return per_source.reshape(GROUP_ROWS, TOP_K).astype(jnp.int32)


def setup_inputs(seed: int = 0, part: int = 0) -> dict:
    root_key = jax.random.key(seed)
    shared_keys = jax.random.split(jax.random.fold_in(root_key, 1), 5)
    part_keys = jax.random.split(jax.random.fold_in(jax.random.fold_in(root_key, 2), part), 7)

    def normal_bf16(sub_key, arr_shape, scale_by):
        return (jax.random.normal(sub_key, arr_shape, jnp.float32) * scale_by).astype(jnp.bfloat16)

    return {
        'x_a': normal_bf16(part_keys[0], (GROUP_ROWS, MODEL_DIM), 1.0),
        'route_a': group_routing(part_keys[1]),
        'gate_a': jax.nn.softmax(jax.random.normal(part_keys[2], (GROUP_ROWS, TOP_K), jnp.float32), axis=-1),
        'h_b': normal_bf16(part_keys[3], (GROUP_ROWS, MODEL_DIM), 1.0),
        'attn_b': normal_bf16(part_keys[4], (GROUP_ROWS, ATTN_DIM), 1.0),
        'route_b': group_routing(part_keys[5]),
        'gate_b': jax.nn.softmax(jax.random.normal(part_keys[6], (GROUP_ROWS, TOP_K), jnp.float32), axis=-1),
        'w_qkv': normal_bf16(shared_keys[0], (MODEL_DIM, QKV_DIM), MODEL_DIM ** -0.5),
        'w_o': normal_bf16(shared_keys[1], (ATTN_DIM, MODEL_DIM), ATTN_DIM ** -0.5),
        'w_gate': normal_bf16(shared_keys[2], (NUM_EXPERTS, MODEL_DIM, FF_DIM), MODEL_DIM ** -0.5),
        'w_up': normal_bf16(shared_keys[3], (NUM_EXPERTS, MODEL_DIM, FF_DIM), MODEL_DIM ** -0.5),
        'w_down': normal_bf16(shared_keys[4], (NUM_EXPERTS, FF_DIM, MODEL_DIM), FF_DIM ** -0.5),
    }


def expert_layer(tokens, route_ids, gate_vals, w_gate, w_up, w_down):
    n_entries = GROUP_ROWS * TOP_K
    per_source = route_ids.reshape(GROUP_DEVS, TOKENS_DEV * TOP_K)
    one_hot = (per_source[:, :, None] == jnp.arange(NUM_EXPERTS)[None, None, :]).astype(jnp.int32)
    slot_rank = jnp.sum((jnp.cumsum(one_hot, axis=1) - 1) * one_hot, axis=2)
    buffer_row = jnp.arange(GROUP_DEVS)[:, None] * CAPACITY + slot_rank
    entry_ids = jnp.arange(n_entries)
    slot_table = jnp.full((NUM_EXPERTS, GROUP_DEVS * CAPACITY), n_entries, jnp.int32)
    slot_table = slot_table.at[per_source.reshape(-1), buffer_row.reshape(-1)].set(entry_ids)
    padded = jnp.concatenate([tokens, jnp.zeros((1, MODEL_DIM), tokens.dtype)], axis=0)

    def one_expert(results, inputs):
        rows_ids, gate_w, up_w, down_w = inputs
        expert_in = padded[rows_ids // TOP_K]
        gate_act = jnp.dot(expert_in, gate_w, preferred_element_type=jnp.float32)
        up_act = jnp.dot(expert_in, up_w, preferred_element_type=jnp.float32)
        hidden = (jax.nn.silu(gate_act) * up_act).astype(jnp.bfloat16)
        expert_out = jnp.dot(hidden, down_w, preferred_element_type=jnp.float32).astype(jnp.bfloat16)
        return results.at[rows_ids].set(expert_out), None

    results = jnp.zeros((n_entries + 1, MODEL_DIM), jnp.bfloat16)
    results = lax.scan(one_expert, results, (slot_table, w_gate, w_up, w_down))[0]
    per_choice = results[:n_entries].reshape(GROUP_ROWS, TOP_K, MODEL_DIM)
    mixture = jnp.zeros((GROUP_ROWS, MODEL_DIM), jnp.float32)
    for choice in range(TOP_K):
        mixture = mixture + gate_vals[:, choice:choice + 1] * per_choice[:, choice].astype(jnp.float32)
    return (tokens.astype(jnp.float32) + mixture).astype(jnp.bfloat16)


def reference(x_a, route_a, gate_a, h_b, attn_b, route_b, gate_b, w_qkv, w_o, w_gate, w_up, w_down):
    out_a = expert_layer(x_a, route_a, gate_a, w_gate, w_up, w_down)
    qkv_b = jnp.dot(h_b, w_qkv, preferred_element_type=jnp.float32).astype(jnp.bfloat16)
    proj_b = jnp.dot(attn_b, w_o, preferred_element_type=jnp.float32).astype(jnp.bfloat16)
    mid_b = (h_b.astype(jnp.float32) + proj_b.astype(jnp.float32)).astype(jnp.bfloat16)
    out_b = expert_layer(mid_b, route_b, gate_b, w_gate, w_up, w_down)
    return (out_a, out_b, qkv_b)
```

```python
import functools

import jax
import jax.numpy as jnp
from jax import lax
from jax.experimental import pallas as pl
from jax.experimental.pallas import tpu as pltpu
from jax.sharding import PartitionSpec as P


WIN = 48
STRIDE = 32
SLOTS = 144
F32 = jnp.float32
BF16 = jnp.bfloat16
VMEM_LIMIT = 60 * 1024 * 1024


def permute(x, bit, n):
    return lax.ppermute(x, 'ep', [(i, i ^ bit) for i in range(n)])


def spread(x, n):
    peer = permute(x, 2, n)
    sib = permute(x, 1, n)
    return (x, sib, peer, permute(peer, 1, n))


def routing_tables(route_ids, gate_vals, local_n, me):
    n_src, tok_n, _ = route_ids.shape
    local = route_ids - me * local_n
    experts = jnp.arange(16)
    hit = (local[..., None] == experts) & (experts < local_n)
    chosen = jnp.any(hit, axis=2)
    gates = jnp.sum(jnp.where(hit, gate_vals[..., None], 0.0), axis=2)
    lower = (jnp.arange(tok_n)[:, None] > jnp.arange(tok_n)[None, :]).astype(BF16)
    rank = jnp.einsum('ut,ste->sue', lower, chosen.astype(BF16), preferred_element_type=F32)
    shift = 4.0 * jnp.arange(n_src, dtype=F32)[:, None, None]
    place = jnp.where(chosen, rank + shift, -1.0)
    return place, gates


def gate_up_kernel(n_mb, e0, ne, *refs):
    x_refs = refs[:4 * n_mb]
    place_refs = refs[4 * n_mb:5 * n_mb]
    wg_ref, wu_ref, h_ref, xs_ref = refs[5 * n_mb:]
    step = pl.program_id(0)
    dim = xs_ref.shape[2]
    ff = wg_ref.shape[2]

    @pl.when(step == 0)
    def _():
        for m in range(n_mb):
            for k in range(4):
                tok_n = x_refs[0].shape[0]
                rows = lax.broadcasted_iota(jnp.int32, (WIN, tok_n), 0).astype(F32)
                picks = [
                    jnp.where(jnp.broadcast_to(place_refs[m][k, e0 + e:e0 + e + 1, :], (WIN, tok_n)) == rows, 1.0, 0.0).astype(BF16)
                    for e in range(ne)
                ]
                pick = jnp.concatenate(picks, axis=0)
                lo = SLOTS * m + STRIDE * k

                def column(c, carry):
                    cols = pl.ds(pl.multiple_of(c * 512, 512), 512)
                    rows_in = jnp.dot(pick, x_refs[4 * m + k][:, cols], preferred_element_type=F32)
                    rows_in = rows_in.astype(BF16).reshape(ne, WIN, 512)
                    if k == 0:
                        xs_ref[:, lo:lo + WIN, cols] = rows_in
                    else:
                        xs_ref[:, lo:lo + 16, cols] += rows_in[:, :16]
                        xs_ref[:, lo + 16:lo + WIN, cols] = rows_in[:, 16:]
                    return carry

                lax.fori_loop(0, dim // 512, column, 0)

    x = xs_ref[step]
    full = (ff // 256) * 256
    for c in range(0, full, 256):
        g = jnp.dot(x, wg_ref[0, :, c:c + 256], preferred_element_type=F32)
        u = jnp.dot(x, wu_ref[0, :, c:c + 256], preferred_element_type=F32)
        h_ref[0, :, c:c + 256] = (jax.nn.silu(g) * u).astype(BF16)
    if full < ff:
        both = jnp.concatenate([wg_ref[0, :, full:], wu_ref[0, :, full:]], axis=1)
        gu = jnp.dot(x, both, preferred_element_type=F32)
        g = gu[:, :ff - full]
        u = gu[:, ff - full:]
        h_ref[0, :, full:] = (jax.nn.silu(g) * u).astype(BF16)


def gate_up(xs, places, w_gate, w_up, e0, ne):
    n_mb = len(xs)
    tok_n, dim = xs[0][0].shape
    ff = w_gate.shape[2]
    rows = n_mb * SLOTS
    whole2 = pl.BlockSpec((tok_n, dim), lambda i: (0, 0), pipeline_mode=pl.Buffered(1))
    whole3 = pl.BlockSpec(places[0].shape, lambda i: (0, 0, 0), pipeline_mode=pl.Buffered(1))
    return pl.pallas_call(
        functools.partial(gate_up_kernel, n_mb, e0, ne),
        grid=(ne,),
        in_specs=[whole2] * (4 * n_mb) + [whole3] * n_mb + [
            pl.BlockSpec((1, dim, ff), lambda i: (e0 + i, 0, 0)),
            pl.BlockSpec((1, dim, ff), lambda i: (e0 + i, 0, 0)),
        ],
        out_specs=pl.BlockSpec((1, rows, ff), lambda i: (i, 0, 0)),
        out_shape=jax.ShapeDtypeStruct((ne, rows, ff), BF16),
        scratch_shapes=[pltpu.VMEM((ne, rows, dim), BF16)],
        compiler_params=pltpu.CompilerParams(vmem_limit_bytes=VMEM_LIMIT, dimension_semantics=('arbitrary',)),
        cost_estimate=pl.CostEstimate(
            flops=ne * 4 * 288 * dim * ff, bytes_accessed=ne * 4 * dim * ff, transcendentals=ne * rows * ff),
    )(*[x for group in xs for x in group], *places, w_gate, w_up)


def mix_tables(place, gates):
    hi = gates.astype(BF16)
    rest = gates - hi.astype(F32)
    mid = rest.astype(BF16)
    low = (rest - mid.astype(F32)).astype(BF16)
    return jnp.concatenate([place.astype(BF16), hi, mid, low], axis=2)


def down_kernel(n_exp, groups, part_rows, *refs):
    h_refs = refs[:len(part_rows)]
    w_ref, mix_ref, z_ref, y_ref, g_ref = refs[len(part_rows):]
    j, q = pl.program_id(0), pl.program_id(1)
    per = n_exp // groups
    width = w_ref.shape[2]

    @pl.when((j == 0) & (q == 0))
    def _():
        lanes = g_ref.shape[3]
        col = lax.broadcasted_iota(jnp.int32, (16, lanes), 1)
        first = WIN * lax.broadcasted_iota(jnp.int32, (16, lanes), 0)
        expand = jnp.where((col >= first) & (col < first + WIN), 1.0, 0.0).astype(BF16)
        offset = jnp.sum(jnp.where((col >= first) & (col < first + WIN), (col - first).astype(F32), 0.0), axis=0, keepdims=True)
        for k in range(4):
            mixed = mix_ref[k]
            place = jnp.dot(mixed[:, :16], expand, preferred_element_type=F32)
            here = place == offset
            for i in range(3):
                part = jnp.dot(mixed[:, 16 * i + 16:16 * i + 32], expand, preferred_element_type=F32)
                g_ref[k, i] = jnp.where(here, part, 0.0).astype(BF16)

    for gi in range(groups):
        @pl.when(q == gi)
        def _():
            for e in range(per):
                expert = gi * per + e
                lo = 0
                for part, (count, first) in enumerate(part_rows):
                    if lo <= expert < lo + count:
                        h = h_refs[part][expert - lo, first:first + SLOTS, :]
                    lo += count
                y = jnp.dot(h, w_ref[e], preferred_element_type=F32)
                y_ref[expert] = y.astype(BF16)

    @pl.when(q == groups - 1)
    def _():
        for k in range(4):
            y = y_ref[:, STRIDE * k:STRIDE * k + WIN, :].reshape(n_exp * WIN, width)
            z = jnp.dot(g_ref[k, 0], y, preferred_element_type=F32)
            z = z + jnp.dot(g_ref[k, 1], y, preferred_element_type=F32)
            z = z + jnp.dot(g_ref[k, 2], y, preferred_element_type=F32)
            z_ref[k] = z


def down_mix(hs, part_rows, w_down, mixed, c0, nc, width):
    n_exp, ff, _ = w_down.shape
    tok_n = mixed.shape[1]
    groups = 3
    per = n_exp // groups

    def whole(a):
        zeros = (0,) * a.ndim
        return pl.BlockSpec(a.shape, lambda j, q: zeros, pipeline_mode=pl.Buffered(1))

    return pl.pallas_call(
        functools.partial(down_kernel, n_exp, groups, part_rows),
        grid=(nc, groups),
        in_specs=[whole(h) for h in hs] + [
            pl.BlockSpec((per, ff, width), lambda j, q: (q, 0, c0 + j)),
            whole(mixed),
        ],
        out_specs=pl.BlockSpec((4, tok_n, width), lambda j, q: (0, 0, j)),
        out_shape=jax.ShapeDtypeStruct((4, tok_n, nc * width), F32),
        scratch_shapes=[
            pltpu.VMEM((n_exp, SLOTS, width), BF16),
            pltpu.VMEM((4, 3, tok_n, n_exp * WIN), BF16),
        ],
        compiler_params=pltpu.CompilerParams(vmem_limit_bytes=VMEM_LIMIT, dimension_semantics=('arbitrary', 'arbitrary')),
        cost_estimate=pl.CostEstimate(
            flops=nc * width * n_exp * 8 * 288 * ff, bytes_accessed=nc * width * n_exp * 2 * ff, transcendentals=0),
    )(*hs, w_down, mixed)


def solution(mesh):
    n = mesh.shape['ep']

    def layer(x_a, route_a, gate_a, h_b, attn_b, route_b, gate_b, w_qkv, w_o, w_gate, w_up, w_down):
        me = lax.axis_index('ep')
        local_n = w_gate.shape[0]
        dim = x_a.shape[1]
        small = jnp.concatenate([route_a.astype(F32), route_b.astype(F32), gate_a, gate_b], axis=1)
        small = jnp.stack(spread(small, n))
        xs_a = spread(x_a, n)
        routes = small[..., :8].astype(jnp.int32)
        place_a, gates_a = routing_tables(routes[..., :4], small[..., 8:12], local_n, me)
        place_b, gates_b = routing_tables(routes[..., 4:], small[..., 12:], local_n, me)
        mixed_a, mixed_b = mix_tables(place_a, gates_a), mix_tables(place_b, gates_b)
        place_a, place_b = place_a.transpose(0, 2, 1), place_b.transpose(0, 2, 1)

        proj_b = jnp.dot(attn_b, w_o, preferred_element_type=F32).astype(BF16)
        u_b = (h_b.astype(F32) + proj_b.astype(F32)).astype(BF16)
        xs_b = spread(u_b, n)
        qkv_b = jnp.dot(h_b, w_qkv, preferred_element_type=F32).astype(BF16)

        split = 7
        width, per_call = 512, 2
        h_a1 = gate_up((xs_a,), (place_a,), w_gate, w_up, 0, split)
        h_ab = gate_up((xs_a, xs_b), (place_a, place_b), w_gate, w_up, split, local_n - split)

        def combine(u, hs, first, mixed):
            outs = []
            parts = ((split, 0), (local_n - split, first))
            for c in range(0, dim // width, per_call):
                z = down_mix(hs, parts, w_down, mixed, c, per_call, width)
                got = permute(z[1::2], 1, n)
                mine = z[0] + got[0]
                there = z[2] + got[1]
                back = permute(there, 2, n)
                lo = c * width
                cols = u[:, lo:lo + per_call * width].astype(F32)
                outs.append((cols + (mine + back)).astype(BF16))
            return jnp.concatenate(outs, axis=1)

        out_a = combine(x_a, (h_a1, h_ab), 0, mixed_a)
        h_b1 = gate_up((xs_b,), (place_b,), w_gate, w_up, 0, split)
        out_b = combine(u_b, (h_b1, h_ab), SLOTS, mixed_b)
        return out_a, out_b, qkv_b

    row_spec = P(('dp', 'ep'), None)
    full_spec = P(None, None)
    expert_spec = P('ep', None, None)
    return jax.shard_map(
        layer,
        mesh=mesh,
        in_specs=(row_spec, row_spec, row_spec, row_spec, row_spec, row_spec, row_spec, full_spec, full_spec, expert_spec, expert_spec, expert_spec),
        out_specs=(row_spec, row_spec, row_spec),
        check_vma=False,
    )
```

```python
import functools

import jax
import jax.numpy as jnp
from jax import lax
from jax.experimental import pallas as pl
from jax.experimental.pallas import tpu as pltpu
from jax.sharding import PartitionSpec as P

F32 = jnp.float32
BF16 = jnp.bfloat16
CAP = 36
STRIDE = 32
WIN = 48
SLOTS = 144
CHUNK = 512
SET = 6
VMEM_LIMIT = 67043328


def dot(a, b):
    return jnp.dot(a, b, preferred_element_type=F32)


def layer_kernel(
    x_hbm, h_hbm, attn_hbm, meta_hbm, wqkv_hbm, wo_hbm, wg_hbm, wu_hbm, wd_hbm,
    mine_hbm, back_hbm, u_hbm, qkv_hbm,
    xv, xs, hh, ring, gm, mv, pt, zs, zr, xsend, mstage,
    ring_sem, tail_sem, load_sem, out_sem, meta_send, meta_recv, row_send, row_recv,
    zs_sem, zr_sem, xsend_sem, back_sem, mine_sem,
):
    tok, dim = x_hbm.shape
    local_n, ff, _ = wd_hbm.shape
    n_first = (local_n + 1) // 2
    n_both = local_n - n_first
    per = 5
    n_col = dim // CHUNK
    me = lax.axis_index('ep')
    sib = {'ep': me + 1 - 2 * lax.rem(me, 2)}
    peer = {'ep': lax.rem(me + 2, 4)}
    mesh_id = pl.DeviceIdType.MESH

    def remote(src, dst, send, recv, who):
        return pltpu.make_async_remote_copy(
            src_ref=src, dst_ref=dst, send_sem=send, recv_sem=recv, device_id=who, device_id_type=mesh_id)

    phases = {
        'o': 1, 'q': wqkv_hbm.shape[1] // (4 * CHUNK), 'ga': n_first, 'gab': n_both,
        'da': n_col * (local_n // per), 'gb': n_first, 'db': n_col * (local_n // per),
    }
    names = list(phases)
    base = {}
    total = 0
    for name in names:
        base[name] = total
        total += phases[name]

    def copies(name, i, half):
        s0 = half * SET
        out = []

        def add(src, slot, rows, lo, hi, sem):
            out.append(pltpu.make_async_copy(src, ring.at[s0 + slot, :rows, lo:hi], sem))

        if name in ('o', 'q'):
            for c in range(4):
                src = wo_hbm if name == 'o' else wqkv_hbm
                cols = pl.ds(pl.multiple_of((4 * i + c) * CHUNK, CHUNK), CHUNK)
                add(src.at[:, cols], c, dim, 0, CHUNK, ring_sem.at[half, c])
        elif name[0] == 'g':
            e = i + (n_first if name == 'gab' else 0)
            for p in range(2):
                cols = slice(p * CHUNK, (p + 1) * CHUNK)
                add(wg_hbm.at[e, :, cols], 2 * p, dim, 0, CHUNK, ring_sem.at[half, 2 * p])
                add(wu_hbm.at[e, :, cols], 2 * p + 1, dim, 0, CHUNK, ring_sem.at[half, 2 * p + 1])
            add(wg_hbm.at[e, :, 1024:1408], 4, dim, 0, 384, ring_sem.at[half, 4])
            add(wu_hbm.at[e, :, 1280:1408], 4, dim, 384, 512, tail_sem.at[half])
            add(wu_hbm.at[e, :, 1024:1280], 5, dim, 0, 256, ring_sem.at[half, 5])
        else:
            j, q = i // (local_n // per), lax.rem(i, local_n // per)
            cols = pl.ds(pl.multiple_of(j * CHUNK, CHUNK), CHUNK)
            for c in range(per):
                add(wd_hbm.at[q * per + c, :, cols], c, ff, 0, CHUNK, ring_sem.at[half, c])
        return out

    def start(name, i, half):
        for c in copies(name, i, half):
            c.start()

    def wait(name, i, half):
        for c in copies(name, i, half):
            c.wait()

    def half_of(name, i):
        return lax.rem(base[name] + i, 2)

    def prefetch(name, i):
        n = phases[name]
        half = half_of(name, i)
        at = names.index(name)

        def later(k):
            if at + 1 < len(names):
                start(names[at + 1], k, half)

        if isinstance(i, int):
            if i + 2 < n:
                start(name, i + 2, half)
            else:
                later(i + 2 - n)
        else:
            @pl.when(i + 2 < n)
            def _():
                start(name, i + 2, half)

            @pl.when(i + 2 >= n)
            def _():
                later(i + 2 - n)

    barrier = pltpu.get_barrier_semaphore()
    for who in (sib, peer):
        pl.semaphore_signal(barrier, inc=1, device_id=who, device_id_type=mesh_id)
    pl.semaphore_wait(barrier, 2)

    loads = [
        pltpu.make_async_copy(attn_hbm, xs.at[0:tok], load_sem.at[0]),
        pltpu.make_async_copy(h_hbm, xs.at[tok:2 * tok], load_sem.at[1]),
        pltpu.make_async_copy(x_hbm, xv.at[0, 0], load_sem.at[2]),
        pltpu.make_async_copy(meta_hbm, mv.at[0], load_sem.at[3]),
    ]
    for c in loads[:2]:
        c.start()
    start('o', 0, 0)
    meta_out = [remote(meta_hbm, mv.at[2], meta_send.at[0], meta_recv.at[0], peer),
                remote(meta_hbm, mv.at[1], meta_send.at[1], meta_recv.at[1], sib)]
    rows_out = [remote(x_hbm, xv.at[0, 2], row_send.at[0, 0], row_recv.at[0, 0], peer),
                remote(x_hbm, xv.at[0, 1], row_send.at[0, 1], row_recv.at[0, 1], sib)]
    for c in meta_out + rows_out:
        c.start()
    for c in loads[2:]:
        c.start()
    start('q', 0, 1)
    for c in loads[:2]:
        c.wait()

    wait('o', 0, 0)
    for c in range(4):
        cols = slice(c * CHUNK, (c + 1) * CHUNK)
        proj = dot(xs[0:tok, :], ring[c]).astype(BF16)
        xv[1, 0, :, cols] = (xs[tok:2 * tok, cols].astype(F32) + proj.astype(F32)).astype(BF16)
    prefetch('o', 0)

    n_q = phases['q']

    def qkv_out(i):
        rows = pl.ds(pl.multiple_of((2 + lax.rem(i, 2)) * tok, tok), tok)
        cols = pl.ds(pl.multiple_of(i * 4 * CHUNK, 4 * CHUNK), 4 * CHUNK)
        return pltpu.make_async_copy(xs.at[rows], qkv_hbm.at[:, cols], out_sem.at[lax.rem(i, 2)])

    def qkv_step(i, carry):
        half = half_of('q', i)
        wait('q', i, half)

        @pl.when(i >= 2)
        def _():
            qkv_out(i - 2).wait()

        rows = pl.ds(pl.multiple_of((2 + lax.rem(i, 2)) * tok, tok), tok)
        for c in range(4):
            out = dot(xs[tok:2 * tok, :], ring[half * SET + c])
            xs[rows, c * CHUNK:(c + 1) * CHUNK] = out.astype(BF16)
        prefetch('q', i)
        qkv_out(i).start()
        return carry

    lax.fori_loop(0, 1, qkv_step, 0)
    u_out = pltpu.make_async_copy(xv.at[1, 0], u_hbm, out_sem.at[2])
    u_out.start()
    rows_out += [remote(xv.at[1, 0], xv.at[1, 2], row_send.at[1, 0], row_recv.at[1, 0], peer),
                 remote(xv.at[1, 0], xv.at[1, 1], row_send.at[1, 1], row_recv.at[1, 1], sib)]
    for c in rows_out[2:]:
        c.start()
    lax.fori_loop(1, n_q, qkv_step, 0)

    meta_out[0].wait_recv()
    meta_out.append(remote(mv.at[2], mv.at[3], meta_send.at[2], meta_recv.at[2], sib))
    meta_out[2].start()
    loads[3].wait()
    meta_out[1].wait_recv()
    meta_out[2].wait_recv()
    for c in meta_out:
        c.wait_send()
    first_expert = (me * local_n).astype(F32)
    expert_rows = lax.broadcasted_iota(jnp.int32, (16, tok), 0).astype(F32)
    before = (lax.broadcasted_iota(jnp.int32, (tok, tok), 0)
              < lax.broadcasted_iota(jnp.int32, (tok, tok), 1)).astype(F32).astype(BF16)
    for k in range(4):
        turned = mv[k].T
        for m in range(2):
            hit = jnp.zeros((16, tok), F32)
            for c in range(4):
                local = turned[4 * m + c:4 * m + c + 1, :] - first_expert
                hit = jnp.where(jnp.broadcast_to(local, (16, tok)) == expert_rows, 1.0, hit)
            rank = dot(hit.astype(BF16), before)
            pt[m, k] = jnp.where(hit > 0.5, rank + 4.0 * k, -1.0)

    def mix_tables(m):
        lanes = gm.shape[3]
        col = lax.broadcasted_iota(jnp.int32, (16, lanes), 1)
        first = WIN * lax.broadcasted_iota(jnp.int32, (16, lanes), 0)
        inside = (col >= first) & (col < first + WIN)
        expand = jnp.where(inside, 1.0, 0.0).astype(BF16)
        offset = jnp.sum(jnp.where(inside, (col - first).astype(F32), 0.0), axis=0, keepdims=True)
        expert_lanes = lax.broadcasted_iota(jnp.int32, (tok, 16), 1).astype(F32)
        after = (lax.broadcasted_iota(jnp.int32, (tok, tok), 0)
                 > lax.broadcasted_iota(jnp.int32, (tok, tok), 1)).astype(F32).astype(BF16)
        for k in range(4):
            hit = jnp.zeros((tok, 16), F32)
            gate = jnp.zeros((tok, 16), F32)
            for c in range(4):
                local = mv[k, :, 4 * m + c:4 * m + c + 1] - first_expert
                same = jnp.broadcast_to(local, (tok, 16)) == expert_lanes
                hit = jnp.where(same, 1.0, hit)
                gate = jnp.where(same, jnp.broadcast_to(mv[k, :, 8 + 4 * m + c:9 + 4 * m + c], (tok, 16)), gate)
            place = jnp.where(hit > 0.5, dot(after, hit.astype(BF16)) + 4.0 * k, -1.0)
            here = dot(place.astype(BF16), expand) == offset
            for i in range(3):
                part = gate.astype(BF16)
                gate = gate - part.astype(F32)
                gm[k, i] = jnp.where(here, dot(part, expand), 0.0).astype(BF16)

    def dispatch(m, k, e0, ne, rows_per, shift):
        rows = lax.broadcasted_iota(jnp.int32, (WIN, tok), 0).astype(F32)
        pick = jnp.concatenate([
            jnp.where(jnp.broadcast_to(pt[m, k, e:e + 1, :], (WIN, tok)) == rows, 1.0, 0.0).astype(BF16)
            for e in range(e0, e0 + ne)], axis=0)
        for c in range(0, dim, CHUNK):
            got = dot(pick, xv[m, k, :, c:c + CHUNK]).astype(BF16)
            for e in range(ne):
                lo = e * rows_per + shift + STRIDE * k
                piece = got[e * WIN:(e + 1) * WIN]
                if k == 0:
                    xs[lo:lo + WIN, c:c + CHUNK] = piece
                else:
                    xs[lo:lo + 16, c:c + CHUNK] += piece[:16]
                    xs[lo + 16:lo + WIN, c:c + CHUNK] = piece[16:]

    def gate_up(name, rows_per, where):
        def step(i, carry):
            half = half_of(name, i)
            s0 = half * SET
            wait(name, i, half)
            rows = pl.ds(pl.multiple_of(i * rows_per, 16), rows_per)

            def put(lo, hi, g, u):
                h = (jax.nn.silu(g) * u).astype(BF16)
                for r, shift in enumerate(where):
                    hh[i + shift, :, lo:hi] = h[r * SLOTS:(r + 1) * SLOTS]

            for p in range(2):
                g = dot(xs[rows, :], ring[s0 + 2 * p])
                u = dot(xs[rows, :], ring[s0 + 2 * p + 1])
                put(p * CHUNK, (p + 1) * CHUNK, g, u)
            t = dot(xs[rows, :], ring[s0 + 4])
            u = dot(xs[rows, :], ring[s0 + 5, :, 0:256])
            put(1024, 1280, t[:, :256], u)
            put(1280, 1408, t[:, 256:384], t[:, 384:512])
            prefetch(name, i)
            return carry

        lax.fori_loop(0, phases[name], step, 0)

    def mine_out(m, j):
        slot = lax.rem(j, 2)
        cols = pl.ds(pl.multiple_of(j * CHUNK, CHUNK), CHUNK)
        return pltpu.make_async_copy(mstage.at[slot], mine_hbm.at[m, :, cols], mine_sem.at[slot])

    def back_out(m, j):
        slot = lax.rem(j, 2)
        cols = pl.ds(pl.multiple_of(j * CHUNK, CHUNK), CHUNK)
        return remote(xsend.at[slot], back_hbm.at[m, :, cols], xsend_sem.at[slot], back_sem.at[m, j], peer)

    def sib_out(j):
        slot = lax.rem(j, 2)
        return remote(zs, zr.at[slot], zs_sem, zr_sem.at[slot], sib)

    def down(name, m):
        groups = local_n // per

        def step(i, carry):
            half = half_of(name, i)
            s0 = half * SET
            j, q = i // groups, lax.rem(i, groups)
            wait(name, i, half)
            for c in range(per):
                e = q * per + c
                y = dot(hh[e + m * n_both], ring[s0 + c, :ff, :])
                xs[pl.ds(pl.multiple_of(e * SLOTS, 16), SLOTS), 0:CHUNK] = y.astype(BF16)
            prefetch(name, i)

            @pl.when(q == groups - 1)
            def _():
                slot = lax.rem(j, 2)

                def mix(k):
                    y = jnp.concatenate(
                        [xs[e * SLOTS + STRIDE * k:e * SLOTS + STRIDE * k + WIN, 0:CHUNK] for e in range(local_n)], axis=0)
                    return dot(gm[k, 0], y) + dot(gm[k, 1], y) + dot(gm[k, 2], y)

                if m == 0:
                    @pl.when(j >= 1)
                    def _():
                        sib_out(j - 1).wait_send()

                    @pl.when(j >= 2)
                    def _():
                        mine_out(0, j - 2).wait()
                        back_out(0, j - 2).wait_send()
                else:
                    sib_out(j + 1).wait_send()
                    mine_out(m, j).wait()
                    back_out(m, j).wait_send()
                zs[0] = mix(1)
                zs[1] = mix(3)
                sib_out(j).start()
                mstage[slot] = mix(0)
                xsend[slot] = mix(2)
                sib_out(j).wait_recv()
                mstage[slot] = mstage[slot] + zr[slot, 0]
                xsend[slot] = xsend[slot] + zr[slot, 1]
                back_out(m, j).start()
                mine_out(m, j).start()

            return carry

        lax.fori_loop(0, phases[name], step, 0)

    def forward(m):
        rows_out[2 * m].wait_recv()
        c = remote(xv.at[m, 2], xv.at[m, 3], row_send.at[m, 2], row_recv.at[m, 2], sib)
        c.start()
        return c

    for i in (n_q - 2, n_q - 1):
        qkv_out(i).wait()
    loads[2].wait()
    rows_out[1].wait_recv()
    dispatch(0, 0, 0, n_first, SLOTS, 0)
    dispatch(0, 1, 0, n_first, SLOTS, 0)
    forward_a = forward(0)
    dispatch(0, 2, 0, n_first, SLOTS, 0)
    forward_a.wait_recv()
    dispatch(0, 3, 0, n_first, SLOTS, 0)
    gate_up('ga', SLOTS, (0,))
    for k in range(4):
        dispatch(0, k, n_first, n_both, 2 * SLOTS, 0)
    rows_out[3].wait_recv()
    dispatch(1, 0, n_first, n_both, 2 * SLOTS, SLOTS)
    dispatch(1, 1, n_first, n_both, 2 * SLOTS, SLOTS)
    forward_b = forward(1)
    dispatch(1, 2, n_first, n_both, 2 * SLOTS, SLOTS)
    mix_tables(0)
    forward_b.wait_recv()
    dispatch(1, 3, n_first, n_both, 2 * SLOTS, SLOTS)
    gate_up('gab', 2 * SLOTS, (n_first, n_first + n_both))
    down('da', 0)
    for k in range(4):
        dispatch(1, k, 0, n_first, SLOTS, 0)
    gate_up('gb', SLOTS, (n_both,))
    mix_tables(1)
    down('db', 1)

    for c in rows_out + [forward_a, forward_b]:
        c.wait_send()
    u_out.wait()
    sib_out(n_col - 1).wait_send()
    for j in (n_col - 2, n_col - 1):
        mine_out(1, j).wait()
        back_out(1, j).wait_send()
    for m in range(2):
        for j in range(n_col):
            back_out(m, j).wait_recv()


def moe_layer(x_a, h_b, attn_b, meta, w_qkv, w_o, w_gate, w_up, w_down):
    tok, dim = x_a.shape
    local_n, ff, _ = w_down.shape
    n_both = local_n - (local_n + 1) // 2
    hbm = pl.BlockSpec(memory_space=pl.ANY)
    dma = pltpu.SemaphoreType.DMA
    flops = 2 * tok * dim * (dim + w_qkv.shape[1]) + local_n * 2 * SLOTS * 6 * dim * ff
    return pl.pallas_call(
        layer_kernel,
        in_specs=[hbm] * 9,
        out_specs=[hbm] * 4,
        out_shape=[
            jax.ShapeDtypeStruct((2, tok, dim), F32),
            jax.ShapeDtypeStruct((2, tok, dim), F32),
            jax.ShapeDtypeStruct((tok, dim), BF16),
            jax.ShapeDtypeStruct((tok, w_qkv.shape[1]), BF16),
        ],
        scratch_shapes=[
            pltpu.VMEM((2, 4, tok, dim), BF16),
            pltpu.VMEM((local_n * SLOTS, dim), BF16),
            pltpu.VMEM((local_n + n_both, SLOTS, ff), BF16),
            pltpu.VMEM((2 * SET, dim, CHUNK), BF16),
            pltpu.VMEM((4, 3, tok, local_n * WIN), BF16),
            pltpu.VMEM((4, tok, 128), F32),
            pltpu.VMEM((2, 4, 16, tok), F32),
            pltpu.VMEM((2, tok, CHUNK), F32),
            pltpu.VMEM((2, 2, tok, CHUNK), F32),
            pltpu.VMEM((2, tok, CHUNK), F32),
            pltpu.VMEM((2, tok, CHUNK), F32),
            dma((2, SET)), dma((2,)), dma((4,)), dma((3,)), dma((3,)), dma((3,)), dma((2, 3)), dma((2, 3)),
            dma(()), dma((2,)), dma((2,)), dma((2, dim // CHUNK)), dma((2,)),
        ],
        compiler_params=pltpu.CompilerParams(
            collective_id=0, has_side_effects=True, vmem_limit_bytes=VMEM_LIMIT),
        cost_estimate=pl.CostEstimate(flops=flops, bytes_accessed=local_n * 6 * dim * ff, transcendentals=0),
        name='moe_layer',
    )(x_a, h_b, attn_b, meta, w_qkv, w_o, w_gate, w_up, w_down)


def solution(mesh):
    def local_step(x_a, route_a, gate_a, h_b, attn_b, route_b, gate_b, w_qkv, w_o, w_gate, w_up, w_down):
        meta = jnp.concatenate([route_a.astype(F32), route_b.astype(F32), gate_a, gate_b], axis=1)
        meta = jnp.pad(meta, ((0, 0), (0, 128 - meta.shape[1])))
        mine, back, u_b, qkv_b = moe_layer(x_a, h_b, attn_b, meta, w_qkv, w_o, w_gate, w_up, w_down)
        out_a = (x_a.astype(F32) + (mine[0] + back[0])).astype(BF16)
        out_b = (u_b.astype(F32) + (mine[1] + back[1])).astype(BF16)
        return out_a, out_b, qkv_b

    row_spec = P(('dp', 'ep'), None)
    full_spec = P(None, None)
    expert_spec = P('ep', None, None)
    return jax.shard_map(
        local_step,
        mesh=mesh,
        in_specs=(row_spec, row_spec, row_spec, row_spec, row_spec, row_spec, row_spec, full_spec, full_spec, expert_spec, expert_spec, expert_spec),
        out_specs=(row_spec, row_spec, row_spec),
        check_vma=False,
    )
```

```python
import functools

import jax
import jax.numpy as jnp
from jax import lax
from jax.experimental import pallas as pl
from jax.experimental.pallas import tpu as pltpu
from jax.sharding import PartitionSpec as P

F32 = jnp.float32
BF16 = jnp.bfloat16
CAP = 36
STRIDE = 32
WIN = 48
SLOTS = 144
CHUNK = 512
SET = 6
VMEM_LIMIT = 67043328


def dot(a, b):
    return jnp.dot(a, b, preferred_element_type=F32)


def layer_kernel(
    x_hbm, h_hbm, attn_hbm, meta_hbm, wqkv_hbm, wo_hbm, wg_hbm, wu_hbm, wd_hbm,
    mine_hbm, back_hbm, outa_hbm, outb_hbm, qkv_hbm,
    xv, xs, hh, ring, gm, mv, pt, zs, zr, xsend, mstage,
    ring_sem, tail_sem, load_sem, out_sem, meta_send, meta_recv, row_send, row_recv,
    zs_sem, zr_sem, xsend_sem, back_sem, mine_sem, last_sem, final_sem,
):
    tok, dim = x_hbm.shape
    local_n, ff, _ = wd_hbm.shape
    n_first = (local_n + 1) // 2
    n_both = local_n - n_first
    per = 5
    n_col = dim // CHUNK
    me = lax.axis_index('ep')
    sib = {'ep': me + 1 - 2 * lax.rem(me, 2)}
    peer = {'ep': lax.rem(me + 2, 4)}
    mesh_id = pl.DeviceIdType.MESH

    def remote(src, dst, send, recv, who):
        return pltpu.make_async_remote_copy(
            src_ref=src, dst_ref=dst, send_sem=send, recv_sem=recv, device_id=who, device_id_type=mesh_id)

    phases = {
        'o': 1, 'q': wqkv_hbm.shape[1] // (4 * CHUNK), 'ga': n_first, 'gab': n_both,
        'mix': n_col * (local_n // per) + n_first, 'db': n_col * (local_n // per),
    }
    groups = local_n // per
    each = n_first // n_col
    names = list(phases)
    base = {}
    total = 0
    for name in names:
        base[name] = total
        total += phases[name]

    def copies(name, i, half):
        s0 = half * SET
        out = []

        def add(src, slot, rows, lo, hi, sem):
            out.append(pltpu.make_async_copy(src, ring.at[s0 + slot, :rows, lo:hi], sem))

        if name in ('o', 'q'):
            for c in range(4):
                src = wo_hbm if name == 'o' else wqkv_hbm
                cols = pl.ds(pl.multiple_of((4 * i + c) * CHUNK, CHUNK), CHUNK)
                add(src.at[:, cols], c, dim, 0, CHUNK, ring_sem.at[half, c])
        elif name[0] == 'g':
            e = i + (n_first if name == 'gab' else 0)
            for p in range(2):
                cols = slice(p * CHUNK, (p + 1) * CHUNK)
                add(wg_hbm.at[e, :, cols], 2 * p, dim, 0, CHUNK, ring_sem.at[half, 2 * p])
                add(wu_hbm.at[e, :, cols], 2 * p + 1, dim, 0, CHUNK, ring_sem.at[half, 2 * p + 1])
            add(wg_hbm.at[e, :, 1024:1408], 4, dim, 0, 384, ring_sem.at[half, 4])
            add(wu_hbm.at[e, :, 1280:1408], 4, dim, 384, 512, tail_sem.at[half])
            add(wu_hbm.at[e, :, 1024:1280], 5, dim, 0, 256, ring_sem.at[half, 5])
        else:
            j, q = i // groups, lax.rem(i, groups)
            cols = pl.ds(pl.multiple_of(j * CHUNK, CHUNK), CHUNK)
            for c in range(per):
                add(wd_hbm.at[q * per + c, :, cols], c, ff, 0, CHUNK, ring_sem.at[half, c])
        return out

    def start(name, i, half):
        for c in copies(name, i, half):
            c.start()

    def wait(name, i, half):
        for c in copies(name, i, half):
            c.wait()

    def half_of(name, i):
        return lax.rem(base[name] + i, 2)

    def prefetch(name, i):
        n = phases[name]
        half = half_of(name, i)
        at = names.index(name)

        def later(k):
            if at + 1 < len(names):
                start({'mix': 'da'}.get(names[at + 1], names[at + 1]), k, half)

        if isinstance(i, int):
            if i + 2 < n:
                start(name, i + 2, half)
            else:
                later(i + 2 - n)
        else:
            @pl.when(i + 2 < n)
            def _():
                start(name, i + 2, half)

            @pl.when(i + 2 >= n)
            def _():
                later(i + 2 - n)

    barrier = pltpu.get_barrier_semaphore()
    for who in (sib, peer):
        pl.semaphore_signal(barrier, inc=1, device_id=who, device_id_type=mesh_id)
    pl.semaphore_wait(barrier, 2)

    base['da'] = base['mix']

    loads = [
        pltpu.make_async_copy(attn_hbm, xs.at[0:tok], load_sem.at[0]),
        pltpu.make_async_copy(h_hbm, xs.at[tok:2 * tok], load_sem.at[1]),
        pltpu.make_async_copy(x_hbm, xv.at[0, 0], load_sem.at[2]),
        pltpu.make_async_copy(meta_hbm, mv.at[0], load_sem.at[3]),
    ]
    for c in loads[:2]:
        c.start()
    start('o', 0, 0)
    meta_out = [remote(meta_hbm, mv.at[2], meta_send.at[0], meta_recv.at[0], peer),
                remote(meta_hbm, mv.at[1], meta_send.at[1], meta_recv.at[1], sib)]
    rows_out = [remote(x_hbm, xv.at[0, 2], row_send.at[0, 0], row_recv.at[0, 0], peer),
                remote(x_hbm, xv.at[0, 1], row_send.at[0, 1], row_recv.at[0, 1], sib)]
    for c in meta_out + rows_out:
        c.start()
    for c in loads[2:]:
        c.start()
    start('q', 0, 1)
    for c in loads[:2]:
        c.wait()

    wait('o', 0, 0)
    for c in range(4):
        cols = slice(c * CHUNK, (c + 1) * CHUNK)
        proj = dot(xs[0:tok, :], ring[c]).astype(BF16)
        xv[1, 0, :, cols] = (xs[tok:2 * tok, cols].astype(F32) + proj.astype(F32)).astype(BF16)
    prefetch('o', 0)

    n_q = phases['q']

    def qkv_out(i):
        rows = pl.ds(pl.multiple_of((2 + lax.rem(i, 2)) * tok, tok), tok)
        cols = pl.ds(pl.multiple_of(i * 4 * CHUNK, 4 * CHUNK), 4 * CHUNK)
        return pltpu.make_async_copy(xs.at[rows], qkv_hbm.at[:, cols], out_sem.at[lax.rem(i, 2)])

    def qkv_step(i, carry):
        half = half_of('q', i)
        wait('q', i, half)

        @pl.when(i >= 2)
        def _():
            qkv_out(i - 2).wait()

        rows = pl.ds(pl.multiple_of((2 + lax.rem(i, 2)) * tok, tok), tok)
        for c in range(4):
            out = dot(xs[tok:2 * tok, :], ring[half * SET + c])
            xs[rows, c * CHUNK:(c + 1) * CHUNK] = out.astype(BF16)
        prefetch('q', i)
        qkv_out(i).start()
        return carry

    lax.fori_loop(0, 1, qkv_step, 0)
    rows_out += [remote(xv.at[1, 0], xv.at[1, 2], row_send.at[1, 0], row_recv.at[1, 0], peer),
                 remote(xv.at[1, 0], xv.at[1, 1], row_send.at[1, 1], row_recv.at[1, 1], sib)]
    for c in rows_out[2:]:
        c.start()
    lax.fori_loop(1, n_q, qkv_step, 0)

    meta_out[0].wait_recv()
    meta_out.append(remote(mv.at[2], mv.at[3], meta_send.at[2], meta_recv.at[2], sib))
    meta_out[2].start()
    loads[3].wait()
    meta_out[1].wait_recv()
    meta_out[2].wait_recv()
    for c in meta_out:
        c.wait_send()
    first_expert = (me * local_n).astype(F32)
    expert_rows = lax.broadcasted_iota(jnp.int32, (16, tok), 0).astype(F32)
    before = (lax.broadcasted_iota(jnp.int32, (tok, tok), 0)
              < lax.broadcasted_iota(jnp.int32, (tok, tok), 1)).astype(F32).astype(BF16)
    for k in range(4):
        for m in range(2):
            hit = jnp.zeros((16, tok), F32)
            gate = jnp.zeros((16, tok), F32)
            for c in range(4 * m, 4 * m + 4):
                local = mv[k, c:c + 1, :] - first_expert
                same = jnp.broadcast_to(local, (16, tok)) == expert_rows
                hit = jnp.where(same, 1.0, hit)
                gate = jnp.where(same, jnp.broadcast_to(mv[k, 8 + c:9 + c, :], (16, tok)), gate)
            rank = dot(hit.astype(BF16), before)
            pt[0, m, k] = jnp.where(hit > 0.5, rank + 4.0 * k, -1.0)
            pt[1, m, k] = gate

    def mix_tables(m):
        lanes = gm.shape[3]
        col = lax.broadcasted_iota(jnp.int32, (16, lanes), 1)
        first = WIN * lax.broadcasted_iota(jnp.int32, (16, lanes), 0)
        inside = (col >= first) & (col < first + WIN)
        expand = jnp.where(inside, 1.0, 0.0).astype(BF16)
        offset = jnp.sum(jnp.where(inside, (col - first).astype(F32), 0.0), axis=0, keepdims=True)
        for k in range(4):
            here = dot(pt[0, m, k].T.astype(BF16), expand) == offset
            gate = pt[1, m, k].T
            for i in range(3):
                part = gate.astype(BF16)
                gate = gate - part.astype(F32)
                gm[k, i] = jnp.where(here, dot(part, expand), 0.0).astype(BF16)

    def dispatch(m, k, e0, ne, rows_per, shift):
        rows = lax.broadcasted_iota(jnp.int32, (WIN, tok), 0).astype(F32)
        pick = jnp.concatenate([
            jnp.where(jnp.broadcast_to(pt[0, m, k, e:e + 1, :], (WIN, tok)) == rows, 1.0, 0.0).astype(BF16)
            for e in range(e0, e0 + ne)], axis=0)
        for c in range(0, dim, CHUNK):
            got = dot(pick, xv[m, k, :, c:c + CHUNK]).astype(BF16)
            for e in range(ne):
                lo = e * rows_per + shift + STRIDE * k
                piece = got[e * WIN:(e + 1) * WIN]
                if k == 0:
                    xs[lo:lo + WIN, c:c + CHUNK] = piece
                else:
                    xs[lo:lo + 16, c:c + CHUNK] += piece[:16]
                    xs[lo + 16:lo + WIN, c:c + CHUNK] = piece[16:]

    def expert_hidden(i, half, rows_per, where):
        s0 = half * SET
        rows = pl.ds(pl.multiple_of(i * rows_per, 16), rows_per)

        def put(lo, hi, g, u):
            h = (jax.nn.silu(g) * u).astype(BF16)
            for r, shift in enumerate(where):
                hh[i + shift, :, lo:hi] = h[r * SLOTS:(r + 1) * SLOTS]

        for p in range(2):
            g = dot(xs[rows, :], ring[s0 + 2 * p])
            u = dot(xs[rows, :], ring[s0 + 2 * p + 1])
            put(p * CHUNK, (p + 1) * CHUNK, g, u)
        t = dot(xs[rows, :], ring[s0 + 4])
        u = dot(xs[rows, :], ring[s0 + 5, :, 0:256])
        put(1024, 1280, t[:, :256], u)
        put(1280, 1408, t[:, 256:384], t[:, 384:512])

    def gate_up(name, rows_per, where):
        def step(i, carry):
            half = half_of(name, i)
            wait(name, i, half)
            expert_hidden(i, half, rows_per, where)
            prefetch(name, i)
            return carry

        lax.fori_loop(0, phases[name], step, 0)

    def mine_out(m, j):
        cols = pl.ds(pl.multiple_of(j * CHUNK, CHUNK), CHUNK)
        return pltpu.make_async_copy(mstage, mine_hbm.at[m, :, cols], mine_sem)

    def back_out(m, j):
        slot = lax.rem(j, 2)
        cols = pl.ds(pl.multiple_of(j * CHUNK, CHUNK), CHUNK)
        return remote(xsend.at[slot], back_hbm.at[m, :, cols], xsend_sem.at[slot], back_sem.at[m, j], peer)

    def sib_out(j):
        slot = lax.rem(j, 2)
        return remote(zs, zr.at[slot], zs_sem, zr_sem.at[slot], sib)

    y_row = n_first * SLOTS
    y_per = local_n - n_first

    def expert_out(m, q, half):
        for c in range(per):
            e = q * per + c
            y = dot(hh[e + m * local_n], ring[half * SET + c, :ff, :])
            rows = pl.ds(pl.multiple_of(y_row + lax.rem(e, y_per) * SLOTS, 16), SLOTS)
            cols = pl.ds(pl.multiple_of((e // y_per) * CHUNK, CHUNK), CHUNK)
            xs[rows, cols] = y.astype(BF16)

    def combine(m, j):
        slot = lax.rem(j, 2)

        def mix(k):
            pieces = []
            for e in range(local_n):
                lo = y_row + (e % y_per) * SLOTS + STRIDE * k
                c = (e // y_per) * CHUNK
                pieces.append(xs[lo:lo + WIN, c:c + CHUNK])
            y = jnp.concatenate(pieces, axis=0)
            return dot(gm[k, 0], y) + dot(gm[k, 1], y) + dot(gm[k, 2], y)

        if m == 0:
            @pl.when(j >= 1)
            def _():
                sib_out(j - 1).wait_send()
                mine_out(0, j - 1).wait()

            @pl.when(j >= 2)
            def _():
                back_out(0, j - 2).wait_send()
        else:
            sib_out(j + 1).wait_send()
            mine_out(m, j).wait()
            back_out(m, j).wait_send()
        zs[0] = mix(1)
        zs[1] = mix(3)
        sib_out(j).start()
        mstage[...] = mix(0)
        xsend[slot] = mix(2)
        sib_out(j).wait_recv()
        mstage[...] = mstage[...] + zr[slot, 0]
        xsend[slot] = xsend[slot] + zr[slot, 1]
        back_out(m, j).start()
        mine_out(m, j).start()

    def down_b(i, carry):
        half = half_of('db', i)
        wait('db', i, half)
        expert_out(1, lax.rem(i, groups), half)
        prefetch('db', i)

        @pl.when(lax.rem(i, groups) == groups - 1)
        def _():
            combine(1, i // groups)

        return carry

    def down_a_gate_b(t, carry):
        first = base['mix'] + t * (groups + each)

        def outputs(q, c2):
            half = lax.rem(first + q, 2)
            wait('da', t * groups + q, half)
            expert_out(0, q, half)

            @pl.when(q + 2 < groups)
            def _():
                start('da', t * groups + q + 2, half)

            @pl.when(q + 2 >= groups)
            def _():
                start('gb', t * each + q + 2 - groups, half)

            return c2

        lax.fori_loop(0, groups, outputs, 0)
        combine(0, t)

        @pl.when(t == 0)
        def _():
            for k in range(4):
                dispatch(1, k, 0, n_first, SLOTS, 0)

        def hidden(r, c2):
            half = lax.rem(first + groups + r, 2)
            e = t * each + r
            wait('gb', e, half)
            expert_hidden(e, half, SLOTS, (local_n,))

            @pl.when(t + 1 < n_col)
            def _():
                start('da', (t + 1) * groups + r, half)

            @pl.when(t + 1 >= n_col)
            def _():
                start('db', r, half)

            return c2

        lax.fori_loop(0, each, hidden, 0)
        return carry

    def forward(m):
        rows_out[2 * m].wait_recv()
        c = remote(xv.at[m, 2], xv.at[m, 3], row_send.at[m, 2], row_recv.at[m, 2], sib)
        c.start()
        return c

    for i in (n_q - 2, n_q - 1):
        qkv_out(i).wait()
    loads[2].wait()
    rows_out[1].wait_recv()
    dispatch(0, 0, 0, n_first, SLOTS, 0)
    dispatch(0, 1, 0, n_first, SLOTS, 0)
    forward_a = forward(0)
    dispatch(0, 2, 0, n_first, SLOTS, 0)
    forward_a.wait_recv()
    dispatch(0, 3, 0, n_first, SLOTS, 0)
    gate_up('ga', SLOTS, (0,))
    for k in range(4):
        dispatch(0, k, n_first, n_both, 2 * SLOTS, 0)
    rows_out[3].wait_recv()
    dispatch(1, 0, n_first, n_both, 2 * SLOTS, SLOTS)
    dispatch(1, 1, n_first, n_both, 2 * SLOTS, SLOTS)
    forward_b = forward(1)
    dispatch(1, 2, n_first, n_both, 2 * SLOTS, SLOTS)
    mix_tables(0)
    forward_b.wait_recv()
    dispatch(1, 3, n_first, n_both, 2 * SLOTS, SLOTS)
    gate_up('gab', 2 * SLOTS, (n_first, local_n + n_first))
    lax.fori_loop(0, n_col, down_a_gate_b, 0)
    mix_tables(1)
    lax.fori_loop(0, phases['db'], down_b, 0)

    sib_out(n_col - 1).wait_send()
    mine_out(1, n_col - 1).wait()
    for j in (n_col - 2, n_col - 1):
        back_out(1, j).wait_send()
    outs = []
    for m in range(2):
        for j in range(n_col):
            slot = j % 2
            cols = slice(j * CHUNK, (j + 1) * CHUNK)
            back_out(m, j).wait_recv()
            parts = [
                pltpu.make_async_copy(mine_hbm.at[m, :, cols], zr.at[slot, 0], final_sem.at[0]),
                pltpu.make_async_copy(back_hbm.at[m, :, cols], zr.at[slot, 1], final_sem.at[1]),
            ]
            for c in parts:
                c.start()
            for c in parts:
                c.wait()
            total_row = xv[m, 0, :, cols].astype(F32) + (zr[slot, 0] + zr[slot, 1])
            xs[m * tok:(m + 1) * tok, cols] = total_row.astype(BF16)
            out = pltpu.make_async_copy(
                xs.at[m * tok:(m + 1) * tok, cols], (outa_hbm, outb_hbm)[m].at[:, cols], last_sem.at[m, j])
            out.start()
            outs.append(out)
    for c in rows_out + [forward_a, forward_b]:
        c.wait_send()
    for c in outs:
        c.wait()


def moe_layer(x_a, h_b, attn_b, meta, w_qkv, w_o, w_gate, w_up, w_down):
    tok, dim = x_a.shape
    local_n, ff, _ = w_down.shape
    hbm = pl.BlockSpec(memory_space=pl.ANY)
    dma = pltpu.SemaphoreType.DMA
    flops = 2 * tok * dim * (dim + w_qkv.shape[1]) + local_n * 2 * SLOTS * 6 * dim * ff
    return pl.pallas_call(
        layer_kernel,
        in_specs=[hbm] * 9,
        out_specs=[hbm] * 5,
        out_shape=[
            jax.ShapeDtypeStruct((2, tok, dim), F32),
            jax.ShapeDtypeStruct((2, tok, dim), F32),
            jax.ShapeDtypeStruct((tok, dim), BF16),
            jax.ShapeDtypeStruct((tok, dim), BF16),
            jax.ShapeDtypeStruct((tok, w_qkv.shape[1]), BF16),
        ],
        scratch_shapes=[
            pltpu.VMEM((2, 4, tok, dim), BF16),
            pltpu.VMEM((local_n * SLOTS, dim), BF16),
            pltpu.VMEM((2 * local_n, SLOTS, ff), BF16),
            pltpu.VMEM((2 * SET, dim, CHUNK), BF16),
            pltpu.VMEM((4, 3, tok, local_n * WIN), BF16),
            pltpu.VMEM((4, 16, tok), F32),
            pltpu.VMEM((2, 2, 4, 16, tok), F32),
            pltpu.VMEM((2, tok, CHUNK), F32),
            pltpu.VMEM((2, 2, tok, CHUNK), F32),
            pltpu.VMEM((2, tok, CHUNK), F32),
            pltpu.VMEM((tok, CHUNK), F32),
            dma((2, SET)), dma((2,)), dma((4,)), dma((2,)), dma((3,)), dma((3,)), dma((2, 3)), dma((2, 3)),
            dma(()), dma((2,)), dma((2,)), dma((2, dim // CHUNK)), dma(()), dma((2, dim // CHUNK)), dma((2,)),
        ],
        compiler_params=pltpu.CompilerParams(
            collective_id=0, has_side_effects=True, vmem_limit_bytes=VMEM_LIMIT),
        cost_estimate=pl.CostEstimate(flops=flops, bytes_accessed=local_n * 6 * dim * ff, transcendentals=0),
        name='moe_layer',
    )(x_a, h_b, attn_b, meta, w_qkv, w_o, w_gate, w_up, w_down)


def solution(mesh):
    def local_step(x_a, route_a, gate_a, h_b, attn_b, route_b, gate_b, w_qkv, w_o, w_gate, w_up, w_down):
        meta = jnp.concatenate([route_a.T.astype(F32), route_b.T.astype(F32), gate_a.T, gate_b.T], axis=0)
        _, _, out_a, out_b, qkv_b = moe_layer(x_a, h_b, attn_b, meta, w_qkv, w_o, w_gate, w_up, w_down)
        return out_a, out_b, qkv_b

    row_spec = P(('dp', 'ep'), None)
    full_spec = P(None, None)
    expert_spec = P('ep', None, None)
    return jax.shard_map(
        local_step,
        mesh=mesh,
        in_specs=(row_spec, row_spec, row_spec, row_spec, row_spec, row_spec, row_spec, full_spec, full_spec, expert_spec, expert_spec, expert_spec),
        out_specs=(row_spec, row_spec, row_spec),
        check_vma=False,
    )
```

```python
import functools

import jax
import jax.numpy as jnp
from jax import lax
from jax.experimental import pallas as pl
from jax.experimental.pallas import tpu as pltpu
from jax.sharding import PartitionSpec as P

F32 = jnp.float32
BF16 = jnp.bfloat16
CAP = 36
STRIDE = 32
WIN = 48
SLOTS = 144
CHUNK = 512
SET = 6
VMEM_LIMIT = 67043328


def dot(a, b):
    return jnp.dot(a, b, preferred_element_type=F32)


def layer_kernel(
    x_hbm, h_hbm, attn_hbm, ra_hbm, rb_hbm, ga_hbm, gb_hbm, wqkv_hbm, wo_hbm, wg_hbm, wu_hbm, wd_hbm,
    mine_hbm, back_hbm, outa_hbm, outb_hbm, qkv_hbm,
    xv, xs, hh, ring, gm, rv, gv, pt, zs, zr, xsend, mstage,
    ring_sem, tail_sem, load_sem, out_sem, meta_send, meta_recv, row_send, row_recv,
    zs_sem, zr_sem, xsend_sem, back_sem, mine_sem, last_sem, final_sem,
):
    tok, dim = x_hbm.shape
    local_n, ff, _ = wd_hbm.shape
    n_first = (local_n + 1) // 2
    n_both = local_n - n_first
    per = 5
    n_col = dim // CHUNK
    me = lax.axis_index('ep')
    sib = {'ep': me + 1 - 2 * lax.rem(me, 2)}
    peer = {'ep': lax.rem(me + 2, 4)}
    mesh_id = pl.DeviceIdType.MESH

    def remote(src, dst, send, recv, who):
        return pltpu.make_async_remote_copy(
            src_ref=src, dst_ref=dst, send_sem=send, recv_sem=recv, device_id=who, device_id_type=mesh_id)

    groups = local_n // per
    each = n_first // n_col
    n_q = wqkv_hbm.shape[1] // (4 * CHUNK)
    base_g = 1 + n_q
    base_mix = base_g + local_n
    base_db = base_mix + n_col * groups + n_first

    def half_at(it):
        return it % 2 if isinstance(it, int) else lax.rem(it, 2)

    def copies(kind, i, half, slots=range(SET)):
        out = []

        def add(src, slot, rows, lo, hi, sem):
            if slot in slots:
                out.append(pltpu.make_async_copy(src, ring.at[half, :rows, slot * CHUNK + lo:slot * CHUNK + hi], sem))

        if kind in ('o', 'q'):
            for c in range(4):
                src = wo_hbm if kind == 'o' else wqkv_hbm
                cols = pl.ds(pl.multiple_of((4 * i + c) * CHUNK, CHUNK), CHUNK)
                add(src.at[:, cols], c, dim, 0, CHUNK, ring_sem.at[half, c])
        elif kind == 'g':
            for p in range(2):
                cols = slice(p * CHUNK, (p + 1) * CHUNK)
                add(wg_hbm.at[i, :, cols], 2 * p, dim, 0, CHUNK, ring_sem.at[half, 2 * p])
                add(wu_hbm.at[i, :, cols], 2 * p + 1, dim, 0, CHUNK, ring_sem.at[half, 2 * p + 1])
            add(wg_hbm.at[i, :, 1024:1408], 4, dim, 0, 384, ring_sem.at[half, 4])
            add(wu_hbm.at[i, :, 1280:1408], 4, dim, 384, 512, tail_sem.at[half])
            add(wu_hbm.at[i, :, 1024:1280], 5, dim, 0, 256, ring_sem.at[half, 5])
        else:
            j, q = i
            cols = pl.ds(pl.multiple_of(j * CHUNK, CHUNK), CHUNK)
            for c in range(per):
                add(wd_hbm.at[q * per + c, :, cols], c, ff, 0, CHUNK, ring_sem.at[half, c])
        return out

    def start(*args):
        for c in copies(*args):
            c.start()

    def wait(*args):
        for c in copies(*args):
            c.wait()

    barrier = pltpu.get_barrier_semaphore()
    for who in (sib, peer):
        pl.semaphore_signal(barrier, inc=1, device_id=who, device_id_type=mesh_id)
    pl.semaphore_wait(barrier, 2)

    loads = [
        pltpu.make_async_copy(attn_hbm, xs.at[0:tok], load_sem.at[0]),
        pltpu.make_async_copy(h_hbm, xs.at[tok:2 * tok], load_sem.at[1]),
        pltpu.make_async_copy(x_hbm, xv.at[0, 0], load_sem.at[2]),
    ]
    meta = [(ra_hbm, rv, 0), (rb_hbm, rv, 1), (ga_hbm, gv, 0), (gb_hbm, gv, 1)]
    for i, (src, dst, m) in enumerate(meta):
        loads.append(pltpu.make_async_copy(src, dst.at[0, m], load_sem.at[3 + i]))
    for c in loads[:2]:
        c.start()
    start('o', 0, 0)
    meta_out = []
    for way, who, place in ((0, peer, 2), (1, sib, 1)):
        for i, (src, dst, m) in enumerate(meta):
            meta_out.append(remote(src, dst.at[place, m], meta_send.at[way, i], meta_recv.at[way, i], who))
    rows_out = [remote(x_hbm, xv.at[0, 2], row_send.at[0, 0], row_recv.at[0, 0], peer),
                remote(x_hbm, xv.at[0, 1], row_send.at[0, 1], row_recv.at[0, 1], sib)]
    for c in meta_out + rows_out:
        c.start()
    for c in loads[2:]:
        c.start()
    start('q', 0, 1)
    for c in loads[:2]:
        c.wait()

    wait('o', 0, 0)
    for c in range(4):
        cols = slice(c * CHUNK, (c + 1) * CHUNK)
        proj = dot(xs[0:tok, :], ring[0, :, cols]).astype(BF16)
        xv[1, 0, :, cols] = (xs[tok:2 * tok, cols].astype(F32) + proj.astype(F32)).astype(BF16)
    start('q', 1, 0)
    u_rows = [remote(xv.at[1, 0], xv.at[1, 2], row_send.at[1, 0], row_recv.at[1, 0], peer),
              remote(xv.at[1, 0], xv.at[1, 1], row_send.at[1, 1], row_recv.at[1, 1], sib)]
    rows_out += u_rows

    def qkv_out(i):
        rows = pl.ds(pl.multiple_of((2 + lax.rem(i, 2)) * tok, tok), tok)
        cols = pl.ds(pl.multiple_of(i * 4 * CHUNK, 4 * CHUNK), 4 * CHUNK)
        return pltpu.make_async_copy(xs.at[rows], qkv_hbm.at[:, cols], out_sem.at[lax.rem(i, 2)])

    def qkv_step(i, carry):
        half = half_at(1 + i)
        wait('q', i, half)

        @pl.when(i >= 2)
        def _():
            qkv_out(i - 2).wait()

        rows = pl.ds(pl.multiple_of((2 + lax.rem(i, 2)) * tok, tok), tok)
        for c in range(4):
            out = dot(xs[tok:2 * tok, :], ring[half, :, c * CHUNK:(c + 1) * CHUNK])
            xs[rows, c * CHUNK:(c + 1) * CHUNK] = out.astype(BF16)

        @pl.when(i + 2 < n_q)
        def _():
            start('q', i + 2, half)

        @pl.when(i + 2 >= n_q)
        def _():
            start('g', i + 2 - n_q, half)

        qkv_out(i).start()

        @pl.when(i == 0)
        def _():
            for c in u_rows:
                c.start()

        return carry

    lax.fori_loop(0, n_q, qkv_step, 0)

    for c in meta_out[:4]:
        c.wait_recv()
    for i, (_, dst, m) in enumerate(meta):
        meta_out.append(remote(dst.at[2, m], dst.at[3, m], meta_send.at[2, i], meta_recv.at[2, i], sib))
        meta_out[-1].start()
    for c in loads[3:]:
        c.wait()
    for c in meta_out[4:]:
        c.wait_recv()
    for c in meta_out:
        c.wait_send()
    first_expert = me * local_n
    expert_rows = lax.broadcasted_iota(jnp.int32, (16, tok), 0)
    before = (lax.broadcasted_iota(jnp.int32, (tok, tok), 0)
              < lax.broadcasted_iota(jnp.int32, (tok, tok), 1)).astype(F32).astype(BF16)
    for k in range(4):
        for m in range(2):
            hit = jnp.zeros((16, tok), F32)
            gate = jnp.zeros((16, tok), F32)
            for c in range(4):
                local = rv[k, m, c:c + 1, :] - first_expert
                same = jnp.broadcast_to(local, (16, tok)) == expert_rows
                hit = jnp.where(same, 1.0, hit)
                gate = jnp.where(same, jnp.broadcast_to(gv[k, m, c:c + 1, :], (16, tok)), gate)
            rank = dot(hit.astype(BF16), before)
            pt[0, m, k] = jnp.where(hit > 0.5, rank + 4.0 * k, -1.0)
            pt[1, m, k] = gate

    def mix_tables(m):
        lanes = gm.shape[3]
        col = lax.broadcasted_iota(jnp.int32, (16, lanes), 1)
        first = WIN * lax.broadcasted_iota(jnp.int32, (16, lanes), 0)
        inside = (col >= first) & (col < first + WIN)
        expand = jnp.where(inside, 1.0, 0.0).astype(BF16)
        offset = jnp.sum(jnp.where(inside, (col - first).astype(F32), 0.0), axis=0, keepdims=True)
        for k in range(4):
            here = dot(pt[0, m, k].T.astype(BF16), expand) == offset
            gate = pt[1, m, k].T
            for i in range(3):
                part = gate.astype(BF16)
                gate = gate - part.astype(F32)
                gm[k, i] = jnp.where(here, dot(part, expand), 0.0).astype(BF16)

    def dispatch(m, k, e0, ne, rows_per, shift):
        rows = lax.broadcasted_iota(jnp.int32, (WIN, tok), 0).astype(F32)
        pick = jnp.concatenate([
            jnp.where(jnp.broadcast_to(pt[0, m, k, e:e + 1, :], (WIN, tok)) == rows, 1.0, 0.0).astype(BF16)
            for e in range(e0, e0 + ne)], axis=0)
        for c in range(0, dim, CHUNK):
            got = dot(pick, xv[m, k, :, c:c + CHUNK]).astype(BF16)
            for e in range(ne):
                lo = e * rows_per + shift + STRIDE * k
                piece = got[e * WIN:(e + 1) * WIN]
                if k == 0:
                    xs[lo:lo + WIN, c:c + CHUNK] = piece
                else:
                    xs[lo:lo + 16, c:c + CHUNK] += piece[:16]
                    xs[lo + 16:lo + WIN, c:c + CHUNK] = piece[16:]

    def expert_hidden(i, half, rows_per, where, refill):
        rows = pl.ds(pl.multiple_of(i * rows_per, 16), rows_per)

        def put(lo, hi, g, u):
            h = (jax.nn.silu(g) * u).astype(BF16)
            for r, shift in enumerate(where):
                hh[i + shift, :, lo:hi] = h[r * SLOTS:(r + 1) * SLOTS]

        for p in range(2):
            g = dot(xs[rows, :], ring[half, :, 2 * p * CHUNK:(2 * p + 1) * CHUNK])
            u = dot(xs[rows, :], ring[half, :, (2 * p + 1) * CHUNK:(2 * p + 2) * CHUNK])
            put(p * CHUNK, (p + 1) * CHUNK, g, u)
            refill((2 * p, 2 * p + 1))
        t = dot(xs[rows, :], ring[half, :, 4 * CHUNK:5 * CHUNK])
        u = dot(xs[rows, :], ring[half, :, 5 * CHUNK:])
        put(1024, 1280, t[:, :256], u)
        put(1280, 1408, t[:, 256:384], t[:, 384:512])
        refill((4, 5))

    def gate_up_a(i, carry):
        half = half_at(base_g + i)
        wait('g', i, half)
        expert_hidden(i, half, SLOTS, (0,), lambda slots: start('g', i + 2, half, slots))
        return carry

    def gate_up_ab(i, carry):
        e = n_first + i
        half = half_at(base_g + e)
        wait('g', e, half)

        def refill(slots):
            if slots[0] == 0:
                return
            ready = range(4) if slots[0] == 2 else range(4, SET)

            @pl.when(e + 2 < local_n)
            def _():
                start('g', e + 2, half, ready)

            @pl.when(e + 2 >= local_n)
            def _():
                start('d', (0, e + 2 - local_n), half, ready)

        expert_hidden(i, half, 2 * SLOTS, (n_first, local_n + n_first), refill)
        return carry

    def mine_out(m, j):
        cols = pl.ds(pl.multiple_of(j * CHUNK, CHUNK), CHUNK)
        return pltpu.make_async_copy(mstage, mine_hbm.at[m, :, cols], mine_sem)

    def back_out(m, j):
        slot = lax.rem(j, 2)
        cols = pl.ds(pl.multiple_of(j * CHUNK, CHUNK), CHUNK)
        return remote(xsend.at[slot], back_hbm.at[m, :, cols], xsend_sem.at[slot], back_sem.at[m, j], peer)

    def sib_out(j):
        slot = lax.rem(j, 2)
        return remote(zs, zr.at[slot], zs_sem, zr_sem.at[slot], sib)

    y_row = n_first * SLOTS
    y_per = local_n - n_first

    def expert_out(m, q, half):
        for c in range(per):
            e = q * per + c
            y = dot(hh[e + m * local_n], ring[half, :ff, c * CHUNK:(c + 1) * CHUNK])
            rows = pl.ds(pl.multiple_of(y_row + lax.rem(e, y_per) * SLOTS, 16), SLOTS)
            cols = pl.ds(pl.multiple_of((e // y_per) * CHUNK, CHUNK), CHUNK)
            xs[rows, cols] = y.astype(BF16)

    def mix(k):
        pieces = []
        for e in range(local_n):
            lo = y_row + (e % y_per) * SLOTS + STRIDE * k
            c = (e // y_per) * CHUNK
            pieces.append(xs[lo:lo + WIN, c:c + CHUNK])
        y = jnp.concatenate(pieces, axis=0)
        return dot(gm[k, 0], y) + dot(gm[k, 1], y) + dot(gm[k, 2], y)

    def to_sibling(m, j):
        if m == 0:
            @pl.when(j >= 1)
            def _():
                sib_out(j - 1).wait_send()
        else:
            sib_out(j + 1).wait_send()
        zs[0] = mix(1)
        zs[1] = mix(3)
        sib_out(j).start()

    def to_peer(m, j):
        slot = lax.rem(j, 2)
        if m == 0:
            @pl.when(j >= 1)
            def _():
                mine_out(0, j - 1).wait()

            @pl.when(j >= 2)
            def _():
                back_out(0, j - 2).wait_send()
        else:
            mine_out(m, j).wait()
            back_out(m, j).wait_send()
        mstage[...] = mix(0)
        xsend[slot] = mix(2)
        sib_out(j).wait_recv()
        xsend[slot] = xsend[slot] + zr[slot, 1]
        back_out(m, j).start()
        mstage[...] = mstage[...] + zr[slot, 0]
        mine_out(m, j).start()

    def down_b(j, carry):
        for q in range(groups):
            half = half_at(base_db + j * groups + q)
            wait('d', (j, q), half)
            expert_out(1, q, half)
            if q + 2 < groups:
                start('d', (j, q + 2), half)
            else:
                @pl.when(j + 1 < n_col)
                def _():
                    start('d', (j + 1, q + 2 - groups), half)
        to_sibling(1, j)
        to_peer(1, j)
        return carry

    def down_a_gate_b(t, carry):
        first = base_mix + t * (groups + each)
        for q in range(groups):
            half = half_at(first + q)
            wait('d', (t, q), half)
            expert_out(0, q, half)
            if q + 2 < groups:
                start('d', (t, q + 2), half)
            else:
                start('g', t * each + q + 2 - groups, half)
        to_sibling(0, t)

        @pl.when(t == 0)
        def _():
            for k in range(4):
                dispatch(1, k, 0, n_first, SLOTS, 0)

        for r in range(each):
            half = half_at(first + groups + r)
            e = t * each + r
            wait('g', e, half)
            expert_hidden(e, half, SLOTS, (local_n,), lambda slots: start('d', (lax.rem(t + 1, n_col), r), half, slots))
            if r == 0:
                to_peer(0, t)

                @pl.when(t == n_col - 1)
                def _():
                    mix_tables(1)

        return carry

    def forward(m):
        rows_out[2 * m].wait_recv()
        c = remote(xv.at[m, 2], xv.at[m, 3], row_send.at[m, 2], row_recv.at[m, 2], sib)
        c.start()
        return c

    for i in (n_q - 2, n_q - 1):
        qkv_out(i).wait()
    loads[2].wait()
    rows_out[1].wait_recv()
    dispatch(0, 0, 0, n_first, SLOTS, 0)
    dispatch(0, 1, 0, n_first, SLOTS, 0)
    forward_a = forward(0)
    dispatch(0, 2, 0, n_first, SLOTS, 0)
    forward_a.wait_recv()
    dispatch(0, 3, 0, n_first, SLOTS, 0)
    lax.fori_loop(0, n_first, gate_up_a, 0)
    for k in range(4):
        dispatch(0, k, n_first, n_both, 2 * SLOTS, 0)
    rows_out[3].wait_recv()
    dispatch(1, 0, n_first, n_both, 2 * SLOTS, SLOTS)
    dispatch(1, 1, n_first, n_both, 2 * SLOTS, SLOTS)
    forward_b = forward(1)
    dispatch(1, 2, n_first, n_both, 2 * SLOTS, SLOTS)
    mix_tables(0)
    forward_b.wait_recv()
    dispatch(1, 3, n_first, n_both, 2 * SLOTS, SLOTS)
    lax.fori_loop(0, n_both, gate_up_ab, 0)
    lax.fori_loop(0, n_col, down_a_gate_b, 0)
    lax.fori_loop(0, n_col, down_b, 0)

    sib_out(n_col - 1).wait_send()
    mine_out(1, n_col - 1).wait()
    for j in (n_col - 2, n_col - 1):
        back_out(1, j).wait_send()
    outs = []
    for m in range(2):
        for j in range(n_col):
            slot = j % 2
            cols = slice(j * CHUNK, (j + 1) * CHUNK)
            back_out(m, j).wait_recv()
            parts = [
                pltpu.make_async_copy(mine_hbm.at[m, :, cols], zr.at[slot, 0], final_sem.at[0]),
                pltpu.make_async_copy(back_hbm.at[m, :, cols], zr.at[slot, 1], final_sem.at[1]),
            ]
            for c in parts:
                c.start()
            for c in parts:
                c.wait()
            total_row = xv[m, 0, :, cols].astype(F32) + (zr[slot, 0] + zr[slot, 1])
            xs[m * tok:(m + 1) * tok, cols] = total_row.astype(BF16)
            out = pltpu.make_async_copy(
                xs.at[m * tok:(m + 1) * tok, cols], (outa_hbm, outb_hbm)[m].at[:, cols], last_sem.at[m, j])
            out.start()
            outs.append(out)
    for c in rows_out + [forward_a, forward_b]:
        c.wait_send()
    for c in outs:
        c.wait()


def moe_layer(x_a, h_b, attn_b, r_a, r_b, g_a, g_b, w_qkv, w_o, w_gate, w_up, w_down):
    tok, dim = x_a.shape
    local_n, ff, _ = w_down.shape
    hbm = pl.BlockSpec(memory_space=pl.ANY)
    dma = pltpu.SemaphoreType.DMA
    flops = 2 * tok * dim * (dim + w_qkv.shape[1]) + local_n * 2 * SLOTS * 6 * dim * ff
    return pl.pallas_call(
        layer_kernel,
        in_specs=[hbm] * 12,
        out_specs=[hbm] * 5,
        out_shape=[
            jax.ShapeDtypeStruct((2, tok, dim), F32),
            jax.ShapeDtypeStruct((2, tok, dim), F32),
            jax.ShapeDtypeStruct((tok, dim), BF16),
            jax.ShapeDtypeStruct((tok, dim), BF16),
            jax.ShapeDtypeStruct((tok, w_qkv.shape[1]), BF16),
        ],
        scratch_shapes=[
            pltpu.VMEM((2, 4, tok, dim), BF16),
            pltpu.VMEM((local_n * SLOTS, dim), BF16),
            pltpu.VMEM((2 * local_n, SLOTS, ff), BF16),
            pltpu.VMEM((2, dim, 5 * CHUNK + 256), BF16),
            pltpu.VMEM((4, 3, tok, local_n * WIN), BF16),
            pltpu.VMEM((4, 2, 4, tok), jnp.int32),
            pltpu.VMEM((4, 2, 4, tok), F32),
            pltpu.VMEM((2, 2, 4, 16, tok), F32),
            pltpu.VMEM((2, tok, CHUNK), F32),
            pltpu.VMEM((2, 2, tok, CHUNK), F32),
            pltpu.VMEM((2, tok, CHUNK), F32),
            pltpu.VMEM((tok, CHUNK), F32),
            dma((2, SET)), dma((2,)), dma((7,)), dma((2,)), dma((3, 4)), dma((3, 4)), dma((2, 3)), dma((2, 3)),
            dma(()), dma((2,)), dma((2,)), dma((2, dim // CHUNK)), dma(()), dma((2, dim // CHUNK)), dma((2,)),
        ],
        compiler_params=pltpu.CompilerParams(
            collective_id=0, has_side_effects=True, vmem_limit_bytes=VMEM_LIMIT),
        cost_estimate=pl.CostEstimate(flops=flops, bytes_accessed=local_n * 6 * dim * ff, transcendentals=0),
        name='moe_layer',
    )(x_a, h_b, attn_b, r_a, r_b, g_a, g_b, w_qkv, w_o, w_gate, w_up, w_down)


def hand_on_kernel(n, *refs):
    ins, outs, bufs = refs[:n], refs[n:2 * n], refs[2 * n:3 * n]
    in_sem, out_sem = refs[3 * n:]
    parts = []
    for a in range(n):
        for p in range(ins[a].shape[1] // 1024):
            parts.append((a, slice(1024 * p, 1024 * (p + 1)), len(parts)))
    gets = [pltpu.make_async_copy(ins[a].at[:, c], bufs[a].at[:, c], in_sem.at[i]) for a, c, i in parts]
    puts = [pltpu.make_async_copy(bufs[a].at[:, c], outs[a].at[:, c], out_sem.at[i]) for a, c, i in parts]
    for g in gets:
        g.start()
    for g, p in zip(gets, puts):
        g.wait()
        p.start()
    for p in puts:
        p.wait()


def hand_on(*arrays):
    n = len(arrays)
    count = sum(a.shape[1] // 1024 for a in arrays)
    hbm = pl.BlockSpec(memory_space=pl.ANY)
    return pl.pallas_call(
        functools.partial(hand_on_kernel, n),
        in_specs=[hbm] * n,
        out_specs=[hbm] * n,
        out_shape=[jax.ShapeDtypeStruct(a.shape, a.dtype) for a in arrays],
        scratch_shapes=[pltpu.VMEM(a.shape, a.dtype) for a in arrays] + [
            pltpu.SemaphoreType.DMA((count,)), pltpu.SemaphoreType.DMA((count,))],
        compiler_params=pltpu.CompilerParams(vmem_limit_bytes=VMEM_LIMIT),
        name='hand_on',
    )(*arrays)


def solution(mesh):
    def local_step(x_a, route_a, gate_a, h_b, attn_b, route_b, gate_b, w_qkv, w_o, w_gate, w_up, w_down):
        _, _, out_a, out_b, qkv_b = moe_layer(
            x_a, h_b, attn_b, route_a.T, route_b.T, gate_a.T, gate_b.T, w_qkv, w_o, w_gate, w_up, w_down)
        out_a, out_b, qkv_b = hand_on(out_a, out_b, qkv_b)
        return out_a, out_b, qkv_b

    row_spec = P(('dp', 'ep'), None)
    full_spec = P(None, None)
    expert_spec = P('ep', None, None)
    return jax.shard_map(
        local_step,
        mesh=mesh,
        in_specs=(row_spec, row_spec, row_spec, row_spec, row_spec, row_spec, row_spec, full_spec, full_spec, expert_spec, expert_spec, expert_spec),
        out_specs=(row_spec, row_spec, row_spec),
        check_vma=False,
    )
```

```python
import functools

import jax
import jax.numpy as jnp
from jax import lax
from jax.experimental import pallas as pl
from jax.experimental.pallas import tpu as pltpu
from jax.sharding import PartitionSpec as P

F32 = jnp.float32
BF16 = jnp.bfloat16
CAP = 36
STRIDE = 32
WIN = 48
SLOTS = 144
CHUNK = 512
SET = 6
VMEM_LIMIT = 67043328


def dot(a, b):
    return jnp.dot(a, b, preferred_element_type=F32)


def layer_kernel(
    x_hbm, h_hbm, attn_hbm, ra_hbm, rb_hbm, ga_hbm, gb_hbm, wqkv_hbm, wo_hbm, wg_hbm, wu_hbm, wd_hbm,
    mine_hbm, back_hbm, outa_hbm, outb_hbm, qkv_hbm, table_hbm,
    xv, xs, hh, ring, gm, rv, gv, pt, zs, zr, xsend, mstage,
    ring_sem, tail_sem, load_sem, out_sem, meta_send, meta_recv, row_send, row_recv,
    zs_sem, zr_sem, xsend_sem, back_sem, mine_sem, last_sem, final_sem, table_sem,
):
    tok, dim = x_hbm.shape
    local_n, ff, _ = wd_hbm.shape
    n_first = local_n // 2
    n_both = local_n - n_first
    per = 5
    n_col = dim // CHUNK
    me = lax.axis_index('ep')
    sib = {'ep': me + 1 - 2 * lax.rem(me, 2)}
    peer = {'ep': lax.rem(me + 2, 4)}
    mesh_id = pl.DeviceIdType.MESH

    def remote(src, dst, send, recv, who):
        return pltpu.make_async_remote_copy(
            src_ref=src, dst_ref=dst, send_sem=send, recv_sem=recv, device_id=who, device_id_type=mesh_id)

    groups = local_n // per
    each = (n_first + n_col - 1) // n_col
    n_q = wqkv_hbm.shape[1] // (4 * CHUNK)
    base_g = 1 + n_q
    base_mix = base_g + local_n
    base_db = base_mix + n_col * groups + n_first

    def half_at(it):
        return it % 2 if isinstance(it, int) else lax.rem(it, 2)

    def copies(kind, i, half, slots=range(SET)):
        out = []

        def add(src, slot, rows, lo, hi, sem):
            if slot in slots:
                out.append(pltpu.make_async_copy(src, ring.at[half, :rows, slot * CHUNK + lo:slot * CHUNK + hi], sem))

        if kind in ('o', 'q'):
            for c in range(4):
                src = wo_hbm if kind == 'o' else wqkv_hbm
                cols = pl.ds(pl.multiple_of((4 * i + c) * CHUNK, CHUNK), CHUNK)
                add(src.at[:, cols], c, dim, 0, CHUNK, ring_sem.at[half, c])
        elif kind == 'g':
            for p in range(2):
                cols = slice(p * CHUNK, (p + 1) * CHUNK)
                add(wg_hbm.at[i, :, cols], 2 * p, dim, 0, CHUNK, ring_sem.at[half, 2 * p])
                add(wu_hbm.at[i, :, cols], 2 * p + 1, dim, 0, CHUNK, ring_sem.at[half, 2 * p + 1])
            add(wg_hbm.at[i, :, 1024:1408], 4, dim, 0, 384, ring_sem.at[half, 4])
            add(wu_hbm.at[i, :, 1280:1408], 4, dim, 384, 512, tail_sem.at[half])
            add(wu_hbm.at[i, :, 1024:1280], 5, dim, 0, 256, ring_sem.at[half, 5])
        else:
            j, q = i
            cols = pl.ds(pl.multiple_of(j * CHUNK, CHUNK), CHUNK)
            for c in range(per):
                add(wd_hbm.at[q * per + c, :, cols], c, ff, 0, CHUNK, ring_sem.at[half, c])
        return out

    def start(*args):
        for c in copies(*args):
            c.start()

    def wait(*args):
        for c in copies(*args):
            c.wait()

    barrier = pltpu.get_barrier_semaphore()
    for who in (sib, peer):
        pl.semaphore_signal(barrier, inc=1, device_id=who, device_id_type=mesh_id)
    pl.semaphore_wait(barrier, 2)

    loads = [
        pltpu.make_async_copy(attn_hbm, xs.at[0:tok], load_sem.at[0]),
        pltpu.make_async_copy(h_hbm, xs.at[tok:2 * tok], load_sem.at[1]),
        pltpu.make_async_copy(x_hbm, xv.at[0, 0], load_sem.at[2]),
    ]
    meta = [(ra_hbm, rv, 0), (rb_hbm, rv, 1), (ga_hbm, gv, 0), (gb_hbm, gv, 1)]
    for i, (src, dst, m) in enumerate(meta):
        loads.append(pltpu.make_async_copy(src, dst.at[0, m], load_sem.at[3 + i]))
    for c in loads[:2]:
        c.start()
    start('o', 0, 0)
    meta_out = []
    for way, who, place in ((0, peer, 2), (1, sib, 1)):
        for i, (src, dst, m) in enumerate(meta):
            meta_out.append(remote(src, dst.at[place, m], meta_send.at[way, i], meta_recv.at[way, i], who))
    rows_out = [remote(x_hbm, xv.at[0, 2], row_send.at[0, 0], row_recv.at[0, 0], peer),
                remote(x_hbm, xv.at[0, 1], row_send.at[0, 1], row_recv.at[0, 1], sib)]
    for c in meta_out + rows_out:
        c.start()
    for c in loads[2:]:
        c.start()
    start('q', 0, 1)
    for c in loads[:2]:
        c.wait()

    wait('o', 0, 0)
    for c in range(4):
        cols = slice(c * CHUNK, (c + 1) * CHUNK)
        proj = dot(xs[0:tok, :], ring[0, :, cols]).astype(BF16)
        xv[1, 0, :, cols] = (xs[tok:2 * tok, cols].astype(F32) + proj.astype(F32)).astype(BF16)
    start('q', 1, 0)
    u_rows = [remote(xv.at[1, 0], xv.at[1, 2], row_send.at[1, 0], row_recv.at[1, 0], peer),
              remote(xv.at[1, 0], xv.at[1, 1], row_send.at[1, 1], row_recv.at[1, 1], sib)]
    rows_out += u_rows

    def qkv_out(i):
        rows = pl.ds(pl.multiple_of((2 + lax.rem(i, 2)) * tok, tok), tok)
        cols = pl.ds(pl.multiple_of(i * 4 * CHUNK, 4 * CHUNK), 4 * CHUNK)
        return pltpu.make_async_copy(xs.at[rows], qkv_hbm.at[:, cols], out_sem.at[lax.rem(i, 2)])

    def qkv_step(i, carry):
        half = half_at(1 + i)
        wait('q', i, half)

        @pl.when(i >= 2)
        def _():
            qkv_out(i - 2).wait()

        rows = pl.ds(pl.multiple_of((2 + lax.rem(i, 2)) * tok, tok), tok)
        for c in range(4):
            out = dot(xs[tok:2 * tok, :], ring[half, :, c * CHUNK:(c + 1) * CHUNK])
            xs[rows, c * CHUNK:(c + 1) * CHUNK] = out.astype(BF16)

        @pl.when(i + 2 < n_q)
        def _():
            start('q', i + 2, half)

        @pl.when(i + 2 >= n_q)
        def _():
            start('g', i + 2 - n_q, half)

        qkv_out(i).start()

        @pl.when(i == 0)
        def _():
            for c in u_rows:
                c.start()

        return carry

    lax.fori_loop(0, n_q, qkv_step, 0)

    for c in meta_out[:4]:
        c.wait_recv()
    for i, (_, dst, m) in enumerate(meta):
        meta_out.append(remote(dst.at[2, m], dst.at[3, m], meta_send.at[2, i], meta_recv.at[2, i], sib))
        meta_out[-1].start()
    for c in loads[3:]:
        c.wait()
    for c in meta_out[4:]:
        c.wait_recv()
    for c in meta_out:
        c.wait_send()
    first_expert = me * local_n
    expert_rows = lax.broadcasted_iota(jnp.int32, (16, tok), 0)
    before = (lax.broadcasted_iota(jnp.int32, (tok, tok), 0)
              < lax.broadcasted_iota(jnp.int32, (tok, tok), 1)).astype(F32).astype(BF16)
    for k in range(4):
        for m in range(2):
            hit = jnp.zeros((16, tok), F32)
            gate = jnp.zeros((16, tok), F32)
            for c in range(4):
                local = rv[k, m, c:c + 1, :] - first_expert
                same = jnp.broadcast_to(local, (16, tok)) == expert_rows
                hit = jnp.where(same, 1.0, hit)
                gate = jnp.where(same, jnp.broadcast_to(gv[k, m, c:c + 1, :], (16, tok)), gate)
            rank = dot(hit.astype(BF16), before)
            pt[0, m, k] = jnp.where(hit > 0.5, rank + 4.0 * k, -1.0)
            pt[1, m, k] = gate

    def mix_table(m, k):
        lanes = gm.shape[3]
        col = lax.broadcasted_iota(jnp.int32, (16, lanes), 1)
        first = WIN * lax.broadcasted_iota(jnp.int32, (16, lanes), 0)
        inside = (col >= first) & (col < first + WIN)
        expand = jnp.where(inside, 1.0, 0.0).astype(BF16)
        offset = jnp.sum(jnp.where(inside, (col - first).astype(F32), 0.0), axis=0, keepdims=True)
        here = dot(pt[0, m, k].T.astype(BF16), expand) == offset
        gate = pt[1, m, k].T
        for i in range(3):
            part = gate.astype(BF16)
            gate = gate - part.astype(F32)
            gm[k, i] = jnp.where(here, dot(part, expand), 0.0).astype(BF16)

    def table_out(k):
        return pltpu.make_async_copy(gm.at[k], table_hbm.at[k], table_sem.at[k])

    def table_back(k):
        return pltpu.make_async_copy(table_hbm.at[k], gm.at[k], table_sem.at[k])

    def dispatch(m, k, e0, ne, rows_per, shift):
        rows = lax.broadcasted_iota(jnp.int32, (WIN, tok), 0).astype(F32)
        pick = jnp.concatenate([
            jnp.where(jnp.broadcast_to(pt[0, m, k, e:e + 1, :], (WIN, tok)) == rows, 1.0, 0.0).astype(BF16)
            for e in range(e0, e0 + ne)], axis=0)
        for c in range(0, dim, CHUNK):
            got = dot(pick, xv[m, k, :, c:c + CHUNK]).astype(BF16)
            for e in range(ne):
                lo = e * rows_per + shift + STRIDE * k
                piece = got[e * WIN:(e + 1) * WIN]
                if k == 0:
                    xs[lo:lo + WIN, c:c + CHUNK] = piece
                else:
                    xs[lo:lo + 16, c:c + CHUNK] += piece[:16]
                    xs[lo + 16:lo + WIN, c:c + CHUNK] = piece[16:]

    def expert_hidden(i, half, rows_per, where, refill):
        rows = pl.ds(pl.multiple_of(i * rows_per, 16), rows_per)

        def put(lo, hi, g, u):
            h = (jax.nn.silu(g) * u).astype(BF16)
            for r, shift in enumerate(where):
                hh[i + shift, :, lo:hi] = h[r * SLOTS:(r + 1) * SLOTS]

        for p in range(2):
            g = dot(xs[rows, :], ring[half, :, 2 * p * CHUNK:(2 * p + 1) * CHUNK])
            u = dot(xs[rows, :], ring[half, :, (2 * p + 1) * CHUNK:(2 * p + 2) * CHUNK])
            put(p * CHUNK, (p + 1) * CHUNK, g, u)
            refill((2 * p, 2 * p + 1))
        t = dot(xs[rows, :], ring[half, :, 4 * CHUNK:5 * CHUNK])
        u = dot(xs[rows, :], ring[half, :, 5 * CHUNK:])
        put(1024, 1280, t[:, :256], u)
        put(1280, 1408, t[:, 256:384], t[:, 384:512])
        refill((4, 5))

    def gate_up_a(i, carry):
        half = half_at(base_g + i)
        wait('g', i, half)
        expert_hidden(i, half, SLOTS, (0,), lambda slots: start('g', i + 2, half, slots))

        @pl.when(i < 4)
        def _():
            mix_table(1, i)
            table_out(i).start()

        @pl.when((i >= 3) & (i < 7))
        def _():
            table_out(i - 3).wait()
            mix_table(0, i - 3)

        return carry

    def gate_up_ab(i, carry):
        e = n_first + i
        half = half_at(base_g + e)
        wait('g', e, half)

        def refill(slots):
            if slots[0] == 0:
                return
            ready = range(4) if slots[0] == 2 else range(4, SET)

            @pl.when(e + 2 < local_n)
            def _():
                start('g', e + 2, half, ready)

            @pl.when(e + 2 >= local_n)
            def _():
                start('d', (0, e + 2 - local_n), half, ready)

        expert_hidden(i, half, 2 * SLOTS, (n_first, local_n + n_first), refill)
        return carry

    def mine_out(m, j):
        cols = pl.ds(pl.multiple_of(j * CHUNK, CHUNK), CHUNK)
        return pltpu.make_async_copy(mstage, mine_hbm.at[m, :, cols], mine_sem)

    def back_out(m, j):
        slot = lax.rem(j, 2)
        cols = pl.ds(pl.multiple_of(j * CHUNK, CHUNK), CHUNK)
        return remote(xsend.at[slot], back_hbm.at[m, :, cols], xsend_sem.at[slot], back_sem.at[m, j], peer)

    def sib_out(j):
        slot = lax.rem(j, 2)
        return remote(zs, zr.at[slot], zs_sem, zr_sem.at[slot], sib)

    y_row = n_first * SLOTS
    y_per = local_n - n_first

    def expert_out(m, q, half):
        for c in range(per):
            e = q * per + c
            y = dot(hh[e + m * local_n], ring[half, :ff, c * CHUNK:(c + 1) * CHUNK])
            rows = pl.ds(pl.multiple_of(y_row + lax.rem(e, y_per) * SLOTS, 16), SLOTS)
            cols = pl.ds(pl.multiple_of((e // y_per) * CHUNK, CHUNK), CHUNK)
            xs[rows, cols] = y.astype(BF16)

    def mix(k):
        pieces = []
        for e in range(local_n):
            lo = y_row + (e % y_per) * SLOTS + STRIDE * k
            c = (e // y_per) * CHUNK
            pieces.append(xs[lo:lo + WIN, c:c + CHUNK])
        y = jnp.concatenate(pieces, axis=0)
        return dot(gm[k, 0], y) + dot(gm[k, 1], y) + dot(gm[k, 2], y)

    def to_sibling(m, j):
        if m == 0:
            @pl.when(j >= 1)
            def _():
                sib_out(j - 1).wait_send()
        else:
            sib_out(j + 1).wait_send()
        zs[0] = mix(1)
        zs[1] = mix(3)
        sib_out(j).start()

    def to_peer(m, j):
        slot = lax.rem(j, 2)
        if m == 0:
            @pl.when(j >= 1)
            def _():
                mine_out(0, j - 1).wait()

            @pl.when(j >= 2)
            def _():
                back_out(0, j - 2).wait_send()
        else:
            mine_out(m, j).wait()
            back_out(m, j).wait_send()
        mstage[...] = mix(0)
        xsend[slot] = mix(2)
        sib_out(j).wait_recv()
        xsend[slot] = xsend[slot] + zr[slot, 1]
        back_out(m, j).start()
        mstage[...] = mstage[...] + zr[slot, 0]
        mine_out(m, j).start()

    def down_b(j, carry):
        for q in range(groups):
            half = half_at(base_db + j * groups + q)
            wait('d', (j, q), half)
            expert_out(1, q, half)
            if q + 2 < groups:
                start('d', (j, q + 2), half)
            else:
                @pl.when(j + 1 < n_col)
                def _():
                    start('d', (j + 1, q + 2 - groups), half)

        @pl.when(j == 0)
        def _():
            for k in range(4):
                table_back(k).wait()

        to_sibling(1, j)
        to_peer(1, j)
        return carry

    def down_a_gate_b(t, carry):
        first = base_mix + t * (groups + each)
        for q in range(groups):
            half = half_at(first + q)
            wait('d', (t, q), half)
            expert_out(0, q, half)
            if q + 2 < groups:
                start('d', (t, q + 2), half)
            elif q + 2 == groups:
                start('g', t * each, half)
            else:
                @pl.when(t * each + 1 < n_first)
                def _():
                    start('g', t * each + 1, half)

                @pl.when(t * each + 1 >= n_first)
                def _():
                    start('d', (0, 0), half)
        to_sibling(0, t)

        @pl.when(t == n_col - 1)
        def _():
            table_back(1).start()
            table_back(3).start()

        @pl.when(t == 0)
        def _():
            for k in range(4):
                dispatch(1, k, 0, n_first, SLOTS, 0)

        to_peer(0, t)

        @pl.when(t == n_col - 1)
        def _():
            table_back(0).start()
            table_back(2).start()

        def hidden(r):
            half = half_at(first + groups + r)
            e = t * each + r
            ahead = r + lax.div(t + 1, n_col)
            wait('g', e, half)
            expert_hidden(
                e, half, SLOTS, (local_n,), lambda slots: start('d', (lax.rem(t + 1, n_col), ahead), half, slots))

        hidden(0)

        @pl.when(t * each + 1 < n_first)
        def _():
            hidden(1)

        return carry

    def forward(m):
        rows_out[2 * m].wait_recv()
        c = remote(xv.at[m, 2], xv.at[m, 3], row_send.at[m, 2], row_recv.at[m, 2], sib)
        c.start()
        return c

    for i in (n_q - 2, n_q - 1):
        qkv_out(i).wait()
    loads[2].wait()
    rows_out[1].wait_recv()
    dispatch(0, 0, 0, n_first, SLOTS, 0)
    dispatch(0, 1, 0, n_first, SLOTS, 0)
    forward_a = forward(0)
    dispatch(0, 2, 0, n_first, SLOTS, 0)
    forward_a.wait_recv()
    dispatch(0, 3, 0, n_first, SLOTS, 0)
    lax.fori_loop(0, n_first, gate_up_a, 0)
    for k in range(4):
        dispatch(0, k, n_first, n_both, 2 * SLOTS, 0)
    rows_out[3].wait_recv()
    dispatch(1, 0, n_first, n_both, 2 * SLOTS, SLOTS)
    dispatch(1, 1, n_first, n_both, 2 * SLOTS, SLOTS)
    forward_b = forward(1)
    dispatch(1, 2, n_first, n_both, 2 * SLOTS, SLOTS)
    forward_b.wait_recv()
    dispatch(1, 3, n_first, n_both, 2 * SLOTS, SLOTS)
    lax.fori_loop(0, n_both, gate_up_ab, 0)
    lax.fori_loop(0, n_col, down_a_gate_b, 0)
    lax.fori_loop(0, n_col, down_b, 0)

    sib_out(n_col - 1).wait_send()
    mine_out(1, n_col - 1).wait()
    outs = []
    for m in range(2):
        for j in range(n_col):
            slot = j % 2
            cols = slice(j * CHUNK, (j + 1) * CHUNK)
            back_out(m, j).wait_recv()
            parts = [
                pltpu.make_async_copy(mine_hbm.at[m, :, cols], zr.at[slot, 0], final_sem.at[0]),
                pltpu.make_async_copy(back_hbm.at[m, :, cols], zr.at[slot, 1], final_sem.at[1]),
            ]
            for c in parts:
                c.start()
            for c in parts:
                c.wait()
            total_row = xv[m, 0, :, cols].astype(F32) + (zr[slot, 0] + zr[slot, 1])
            xs[m * tok:(m + 1) * tok, cols] = total_row.astype(BF16)
            out = pltpu.make_async_copy(
                xs.at[m * tok:(m + 1) * tok, cols], (outa_hbm, outb_hbm)[m].at[:, cols], last_sem.at[m, j])
            out.start()
            outs.append(out)
    for j in (n_col - 2, n_col - 1):
        back_out(1, j).wait_send()
    for c in rows_out + [forward_a, forward_b]:
        c.wait_send()
    for c in outs:
        c.wait()


def moe_layer(x_a, h_b, attn_b, r_a, r_b, g_a, g_b, w_qkv, w_o, w_gate, w_up, w_down):
    tok, dim = x_a.shape
    local_n, ff, _ = w_down.shape
    hbm = pl.BlockSpec(memory_space=pl.ANY)
    dma = pltpu.SemaphoreType.DMA
    flops = 2 * tok * dim * (dim + w_qkv.shape[1]) + local_n * 2 * SLOTS * 6 * dim * ff
    return pl.pallas_call(
        layer_kernel,
        in_specs=[hbm] * 12,
        out_specs=[hbm] * 6,
        out_shape=[
            jax.ShapeDtypeStruct((2, tok, dim), F32),
            jax.ShapeDtypeStruct((2, tok, dim), F32),
            jax.ShapeDtypeStruct((tok, dim), BF16),
            jax.ShapeDtypeStruct((tok, dim), BF16),
            jax.ShapeDtypeStruct((tok, w_qkv.shape[1]), BF16),
            jax.ShapeDtypeStruct((4, 3, tok, local_n * WIN), BF16),
        ],
        scratch_shapes=[
            pltpu.VMEM((2, 4, tok, dim), BF16),
            pltpu.VMEM(((local_n + local_n % 2) * SLOTS, dim), BF16),
            pltpu.VMEM((2 * local_n, SLOTS, ff), BF16),
            pltpu.VMEM((2, dim, 5 * CHUNK + 256), BF16),
            pltpu.VMEM((4, 3, tok, local_n * WIN), BF16),
            pltpu.VMEM((4, 2, 4, tok), jnp.int32),
            pltpu.VMEM((4, 2, 4, tok), F32),
            pltpu.VMEM((2, 2, 4, 16, tok), F32),
            pltpu.VMEM((2, tok, CHUNK), F32),
            pltpu.VMEM((2, 2, tok, CHUNK), F32),
            pltpu.VMEM((2, tok, CHUNK), F32),
            pltpu.VMEM((tok, CHUNK), F32),
            dma((2, SET)), dma((2,)), dma((7,)), dma((2,)), dma((3, 4)), dma((3, 4)), dma((2, 3)), dma((2, 3)),
            dma(()), dma((2,)), dma((2,)), dma((2, dim // CHUNK)), dma(()), dma((2, dim // CHUNK)), dma((2,)), dma((4,)),
        ],
        compiler_params=pltpu.CompilerParams(
            collective_id=0, has_side_effects=True, vmem_limit_bytes=VMEM_LIMIT),
        cost_estimate=pl.CostEstimate(flops=flops, bytes_accessed=local_n * 6 * dim * ff, transcendentals=0),
        name='moe_layer',
    )(x_a, h_b, attn_b, r_a, r_b, g_a, g_b, w_qkv, w_o, w_gate, w_up, w_down)


def hand_on_kernel(n, *refs):
    ins, outs, bufs = refs[:n], refs[n:2 * n], refs[2 * n:3 * n]
    in_sem, out_sem = refs[3 * n:]
    parts = []
    for a in range(n):
        for p in range(ins[a].shape[1] // 1024):
            parts.append((a, slice(1024 * p, 1024 * (p + 1)), len(parts)))
    gets = [pltpu.make_async_copy(ins[a].at[:, c], bufs[a].at[:, c], in_sem.at[i]) for a, c, i in parts]
    puts = [pltpu.make_async_copy(bufs[a].at[:, c], outs[a].at[:, c], out_sem.at[i]) for a, c, i in parts]
    for g in gets:
        g.start()
    for g, p in zip(gets, puts):
        g.wait()
        p.start()
    for p in puts:
        p.wait()


def hand_on(*arrays):
    n = len(arrays)
    count = sum(a.shape[1] // 1024 for a in arrays)
    hbm = pl.BlockSpec(memory_space=pl.ANY)
    return pl.pallas_call(
        functools.partial(hand_on_kernel, n),
        in_specs=[hbm] * n,
        out_specs=[hbm] * n,
        out_shape=[jax.ShapeDtypeStruct(a.shape, a.dtype) for a in arrays],
        scratch_shapes=[pltpu.VMEM(a.shape, a.dtype) for a in arrays] + [
            pltpu.SemaphoreType.DMA((count,)), pltpu.SemaphoreType.DMA((count,))],
        compiler_params=pltpu.CompilerParams(vmem_limit_bytes=VMEM_LIMIT),
        name='hand_on',
    )(*arrays)


def solution(mesh):
    def local_step(x_a, route_a, gate_a, h_b, attn_b, route_b, gate_b, w_qkv, w_o, w_gate, w_up, w_down):
        _, _, out_a, out_b, qkv_b, _ = moe_layer(
            x_a, h_b, attn_b, route_a.T, route_b.T, gate_a.T, gate_b.T, w_qkv, w_o, w_gate, w_up, w_down)
        out_a, out_b, qkv_b = hand_on(out_a, out_b, qkv_b)
        return out_a, out_b, qkv_b

    row_spec = P(('dp', 'ep'), None)
    full_spec = P(None, None)
    expert_spec = P('ep', None, None)
    return jax.shard_map(
        local_step,
        mesh=mesh,
        in_specs=(row_spec, row_spec, row_spec, row_spec, row_spec, row_spec, row_spec, full_spec, full_spec, expert_spec, expert_spec, expert_spec),
        out_specs=(row_spec, row_spec, row_spec),
        check_vma=False,
    )
```

```python
import functools

import jax
import jax.numpy as jnp
from jax import lax
from jax.experimental import pallas as pl
from jax.experimental.pallas import tpu as pltpu
from jax.sharding import PartitionSpec as P

F32 = jnp.float32
BF16 = jnp.bfloat16
CAP = 36
STRIDE = 32
WIN = 48
SLOTS = 144
CHUNK = 512
SET = 6
VMEM_LIMIT = 67043328


def dot(a, b):
    return jnp.dot(a, b, preferred_element_type=F32)


def layer_kernel(
    x_hbm, h_hbm, attn_hbm, ra_hbm, rb_hbm, ga_hbm, gb_hbm, wqkv_hbm, wo_hbm, wg_hbm, wu_hbm, wd_hbm,
    mine_hbm, back_hbm, outa_hbm, outb_hbm, qkv_hbm, table_hbm,
    xv, xs, hh, ring, gm, rv, gv, pt, zs, zr, xsend, mstage,
    ring_sem, tail_sem, load_sem, out_sem, meta_send, meta_recv, row_send, row_recv,
    zs_sem, zr_sem, xsend_sem, back_sem, mine_sem, last_sem, final_sem, table_sem, early_sem,
):
    tok, dim = x_hbm.shape
    local_n, ff, _ = wd_hbm.shape
    n_first = local_n // 2
    n_both = local_n - n_first
    per = 5
    n_col = dim // CHUNK
    me = lax.axis_index('ep')
    sib = {'ep': me + 1 - 2 * lax.rem(me, 2)}
    peer = {'ep': lax.rem(me + 2, 4)}
    mesh_id = pl.DeviceIdType.MESH

    def remote(src, dst, send, recv, who):
        return pltpu.make_async_remote_copy(
            src_ref=src, dst_ref=dst, send_sem=send, recv_sem=recv, device_id=who, device_id_type=mesh_id)

    groups = local_n // per
    each = (n_first + n_col - 1) // n_col
    n_q = wqkv_hbm.shape[1] // (4 * CHUNK)
    base_g = 1 + n_q
    base_mix = base_g + local_n - 1
    base_db = base_mix + n_col * groups + n_first

    def half_at(it):
        return it % 2 if isinstance(it, int) else lax.rem(it, 2)

    def copies(kind, i, half, slots=range(SET)):
        out = []

        def add(src, slot, rows, lo, hi, sem):
            if slot in slots:
                out.append(pltpu.make_async_copy(src, ring.at[half, :rows, slot * CHUNK + lo:slot * CHUNK + hi], sem))

        if kind in ('o', 'q'):
            for c in range(4):
                src = wo_hbm if kind == 'o' else wqkv_hbm
                cols = pl.ds(pl.multiple_of((4 * i + c) * CHUNK, CHUNK), CHUNK)
                add(src.at[:, cols], c, dim, 0, CHUNK, ring_sem.at[half, c])
        elif kind == 'g':
            for p in range(2):
                cols = slice(p * CHUNK, (p + 1) * CHUNK)
                add(wg_hbm.at[i, :, cols], 2 * p, dim, 0, CHUNK, ring_sem.at[half, 2 * p])
                add(wu_hbm.at[i, :, cols], 2 * p + 1, dim, 0, CHUNK, ring_sem.at[half, 2 * p + 1])
            add(wg_hbm.at[i, :, 1024:1408], 4, dim, 0, 384, ring_sem.at[half, 4])
            add(wu_hbm.at[i, :, 1280:1408], 4, dim, 384, 512, tail_sem.at[half])
            add(wu_hbm.at[i, :, 1024:1280], 5, dim, 0, 256, ring_sem.at[half, 5])
        else:
            j, q = i
            cols = pl.ds(pl.multiple_of(j * CHUNK, CHUNK), CHUNK)
            for c in range(per):
                add(wd_hbm.at[q * per + c, :, cols], c, ff, 0, CHUNK, ring_sem.at[half, c])
        return out

    def start(*args):
        for c in copies(*args):
            c.start()

    def wait(*args):
        for c in copies(*args):
            c.wait()

    barrier = pltpu.get_barrier_semaphore()
    for who in (sib, peer):
        pl.semaphore_signal(barrier, inc=1, device_id=who, device_id_type=mesh_id)
    pl.semaphore_wait(barrier, 2)

    loads = [
        pltpu.make_async_copy(attn_hbm, xs.at[0:tok], load_sem.at[0]),
        pltpu.make_async_copy(h_hbm, xs.at[tok:2 * tok], load_sem.at[1]),
        pltpu.make_async_copy(x_hbm, xv.at[0, 0], load_sem.at[2]),
    ]
    meta = [(ra_hbm, rv, 0), (rb_hbm, rv, 1), (ga_hbm, gv, 0), (gb_hbm, gv, 1)]
    for i, (src, dst, m) in enumerate(meta):
        loads.append(pltpu.make_async_copy(src, dst.at[0, m], load_sem.at[3 + i]))
    for c in loads[:2]:
        c.start()
    start('o', 0, 0)
    meta_out = []
    for way, who, place in ((0, peer, 2), (1, sib, 1)):
        for i, (src, dst, m) in enumerate(meta):
            meta_out.append(remote(src, dst.at[place, m], meta_send.at[way, i], meta_recv.at[way, i], who))
    rows_out = [remote(x_hbm, xv.at[0, 2], row_send.at[0, 0], row_recv.at[0, 0], peer),
                remote(x_hbm, xv.at[0, 1], row_send.at[0, 1], row_recv.at[0, 1], sib)]
    for c in meta_out + rows_out:
        c.start()
    for c in loads[2:]:
        c.start()
    start('q', 0, 1)
    for c in loads[:2]:
        c.wait()

    wait('o', 0, 0)
    for c in range(4):
        cols = slice(c * CHUNK, (c + 1) * CHUNK)
        proj = dot(xs[0:tok, :], ring[0, :, cols]).astype(BF16)
        xv[1, 0, :, cols] = (xs[tok:2 * tok, cols].astype(F32) + proj.astype(F32)).astype(BF16)
    start('q', 1, 0)
    u_rows = [remote(xv.at[1, 0], xv.at[1, 2], row_send.at[1, 0], row_recv.at[1, 0], peer),
              remote(xv.at[1, 0], xv.at[1, 1], row_send.at[1, 1], row_recv.at[1, 1], sib)]
    rows_out += u_rows

    def qkv_out(i):
        rows = pl.ds(pl.multiple_of((2 + lax.rem(i, 2)) * tok, tok), tok)
        cols = pl.ds(pl.multiple_of(i * 4 * CHUNK, 4 * CHUNK), 4 * CHUNK)
        return pltpu.make_async_copy(xs.at[rows], qkv_hbm.at[:, cols], out_sem.at[lax.rem(i, 2)])

    def qkv_step(i, carry):
        half = half_at(1 + i)
        wait('q', i, half)

        @pl.when(i >= 2)
        def _():
            qkv_out(i - 2).wait()

        rows = pl.ds(pl.multiple_of((2 + lax.rem(i, 2)) * tok, tok), tok)
        for c in range(4):
            out = dot(xs[tok:2 * tok, :], ring[half, :, c * CHUNK:(c + 1) * CHUNK])
            xs[rows, c * CHUNK:(c + 1) * CHUNK] = out.astype(BF16)

        @pl.when(i + 2 < n_q)
        def _():
            start('q', i + 2, half)

        @pl.when(i + 2 >= n_q)
        def _():
            start('g', i + 3 - n_q, half)

        qkv_out(i).start()

        @pl.when(i == 0)
        def _():
            for c in u_rows:
                c.start()

        return carry

    lax.fori_loop(0, n_q, qkv_step, 0)
    early = [pltpu.make_async_copy(wg_hbm.at[0], hh.at[0:dim], early_sem.at[0]),
             pltpu.make_async_copy(wu_hbm.at[0], hh.at[dim:2 * dim], early_sem.at[1])]
    for c in early:
        c.start()

    for c in meta_out[:4]:
        c.wait_recv()
    for i, (_, dst, m) in enumerate(meta):
        meta_out.append(remote(dst.at[2, m], dst.at[3, m], meta_send.at[2, i], meta_recv.at[2, i], sib))
        meta_out[-1].start()
    for c in loads[3:]:
        c.wait()
    for c in meta_out[4:]:
        c.wait_recv()
    for c in meta_out:
        c.wait_send()
    first_expert = me * local_n
    expert_rows = lax.broadcasted_iota(jnp.int32, (16, tok), 0)
    before = (lax.broadcasted_iota(jnp.int32, (tok, tok), 0)
              < lax.broadcasted_iota(jnp.int32, (tok, tok), 1)).astype(F32).astype(BF16)
    for k in range(4):
        for m in range(2):
            hit = jnp.zeros((16, tok), F32)
            gate = jnp.zeros((16, tok), F32)
            for c in range(4):
                local = rv[k, m, c:c + 1, :] - first_expert
                same = jnp.broadcast_to(local, (16, tok)) == expert_rows
                hit = jnp.where(same, 1.0, hit)
                gate = jnp.where(same, jnp.broadcast_to(gv[k, m, c:c + 1, :], (16, tok)), gate)
            rank = dot(hit.astype(BF16), before)
            pt[0, m, k] = jnp.where(hit > 0.5, rank + 4.0 * k, -1.0)
            pt[1, m, k] = gate

    def mix_table(m, k):
        lanes = gm.shape[3]
        col = lax.broadcasted_iota(jnp.int32, (16, lanes), 1)
        first = WIN * lax.broadcasted_iota(jnp.int32, (16, lanes), 0)
        inside = (col >= first) & (col < first + WIN)
        expand = jnp.where(inside, 1.0, 0.0).astype(BF16)
        offset = jnp.sum(jnp.where(inside, (col - first).astype(F32), 0.0), axis=0, keepdims=True)
        here = dot(pt[0, m, k].T.astype(BF16), expand) == offset
        gate = pt[1, m, k].T
        for i in range(3):
            part = gate.astype(BF16)
            gate = gate - part.astype(F32)
            gm[k, i] = jnp.where(here, dot(part, expand), 0.0).astype(BF16)

    def table_out(k):
        return pltpu.make_async_copy(gm.at[k], table_hbm.at[k], table_sem.at[k])

    def table_back(k):
        return pltpu.make_async_copy(table_hbm.at[k], gm.at[k], table_sem.at[k])

    def dispatch(m, k, e0, ne, rows_per, shift):
        rows = lax.broadcasted_iota(jnp.int32, (WIN, tok), 0).astype(F32)
        pick = jnp.concatenate([
            jnp.where(jnp.broadcast_to(pt[0, m, k, e:e + 1, :], (WIN, tok)) == rows, 1.0, 0.0).astype(BF16)
            for e in range(e0, e0 + ne)], axis=0)
        for c in range(0, dim, CHUNK):
            got = dot(pick, xv[m, k, :, c:c + CHUNK]).astype(BF16)
            for e in range(ne):
                lo = e * rows_per + shift + STRIDE * k
                piece = got[e * WIN:(e + 1) * WIN]
                if k == 0:
                    xs[lo:lo + WIN, c:c + CHUNK] = piece
                else:
                    xs[lo:lo + 16, c:c + CHUNK] += piece[:16]
                    xs[lo + 16:lo + WIN, c:c + CHUNK] = piece[16:]

    def hidden_rows(i):
        return pl.ds(pl.multiple_of(i * SLOTS, 16), SLOTS)

    def first_hidden():
        for c in early:
            c.wait()
        x = slice(0, SLOTS)
        spare = slice(n_first * SLOTS, (n_first + 1) * SLOTS)
        for lo in range(0, ff, CHUNK):
            hi = min(lo + CHUNK, ff)
            g = dot(xs[x, :], hh[0:dim, lo:hi])
            u = dot(xs[x, :], hh[dim:2 * dim, lo:hi])
            xs[spare, lo:hi] = (jax.nn.silu(g) * u).astype(BF16)
        hh[0:SLOTS, :] = xs[spare, 0:ff]
        mix_table(1, 0)
        table_out(0).start()

    def expert_hidden(i, half, rows_per, where, refill):
        rows = pl.ds(pl.multiple_of(i * rows_per, 16), rows_per)

        def put(lo, hi, g, u):
            h = (jax.nn.silu(g) * u).astype(BF16)
            for r, shift in enumerate(where):
                hh[hidden_rows(i + shift), lo:hi] = h[r * SLOTS:(r + 1) * SLOTS]

        for p in range(2):
            g = dot(xs[rows, :], ring[half, :, 2 * p * CHUNK:(2 * p + 1) * CHUNK])
            u = dot(xs[rows, :], ring[half, :, (2 * p + 1) * CHUNK:(2 * p + 2) * CHUNK])
            put(p * CHUNK, (p + 1) * CHUNK, g, u)
            refill((2 * p, 2 * p + 1))
        t = dot(xs[rows, :], ring[half, :, 4 * CHUNK:5 * CHUNK])
        u = dot(xs[rows, :], ring[half, :, 5 * CHUNK:])
        put(1024, 1280, t[:, :256], u)
        put(1280, 1408, t[:, 256:384], t[:, 384:512])
        refill((4, 5))

    def gate_up_a(i, carry):
        half = half_at(base_g + i - 1)
        wait('g', i, half)
        expert_hidden(i, half, SLOTS, (0,), lambda slots: start('g', i + 2, half, slots))

        @pl.when(i < 4)
        def _():
            mix_table(1, i)
            table_out(i).start()

        @pl.when((i >= 3) & (i < 7))
        def _():
            table_out(i - 3).wait()
            mix_table(0, i - 3)

        return carry

    def gate_up_ab(i, carry):
        e = n_first + i
        half = half_at(base_g + e - 1)
        wait('g', e, half)

        def refill(slots):
            if slots[0] == 0:
                return
            ready = range(4) if slots[0] == 2 else range(4, SET)

            @pl.when(e + 2 < local_n)
            def _():
                start('g', e + 2, half, ready)

            @pl.when(e + 2 >= local_n)
            def _():
                start('d', (0, e + 2 - local_n), half, ready)

        expert_hidden(i, half, 2 * SLOTS, (n_first, local_n + n_first), refill)
        return carry

    def mine_out(m, j):
        cols = pl.ds(pl.multiple_of(j * CHUNK, CHUNK), CHUNK)
        return pltpu.make_async_copy(mstage, mine_hbm.at[m, :, cols], mine_sem)

    def back_out(m, j):
        slot = lax.rem(j, 2)
        cols = pl.ds(pl.multiple_of(j * CHUNK, CHUNK), CHUNK)
        return remote(xsend.at[slot], back_hbm.at[m, :, cols], xsend_sem.at[slot], back_sem.at[m, j], peer)

    def sib_out(j):
        slot = lax.rem(j, 2)
        return remote(zs, zr.at[slot], zs_sem, zr_sem.at[slot], sib)

    y_row = n_first * SLOTS
    y_per = local_n - n_first

    def expert_out(m, q, half):
        for c in range(per):
            e = q * per + c
            y = dot(hh[hidden_rows(e + m * local_n), :], ring[half, :ff, c * CHUNK:(c + 1) * CHUNK])
            rows = pl.ds(pl.multiple_of(y_row + lax.rem(e, y_per) * SLOTS, 16), SLOTS)
            cols = pl.ds(pl.multiple_of((e // y_per) * CHUNK, CHUNK), CHUNK)
            xs[rows, cols] = y.astype(BF16)

    def mix(k):
        pieces = []
        for e in range(local_n):
            lo = y_row + (e % y_per) * SLOTS + STRIDE * k
            c = (e // y_per) * CHUNK
            pieces.append(xs[lo:lo + WIN, c:c + CHUNK])
        y = jnp.concatenate(pieces, axis=0)
        return dot(gm[k, 0], y) + dot(gm[k, 1], y) + dot(gm[k, 2], y)

    def to_sibling(m, j):
        if m == 0:
            @pl.when(j >= 1)
            def _():
                sib_out(j - 1).wait_send()
        else:
            sib_out(j + 1).wait_send()
        zs[0] = mix(1)
        zs[1] = mix(3)
        sib_out(j).start()

    def to_peer(m, j):
        slot = lax.rem(j, 2)
        if m == 0:
            @pl.when(j >= 1)
            def _():
                mine_out(0, j - 1).wait()

            @pl.when(j >= 2)
            def _():
                back_out(0, j - 2).wait_send()
        else:
            mine_out(m, j).wait()
            back_out(m, j).wait_send()
        mstage[...] = mix(0)
        xsend[slot] = mix(2)
        sib_out(j).wait_recv()
        xsend[slot] = xsend[slot] + zr[slot, 1]
        back_out(m, j).start()
        mstage[...] = mstage[...] + zr[slot, 0]
        mine_out(m, j).start()

    def down_b(j, carry):
        for q in range(groups):
            half = half_at(base_db + j * groups + q)
            wait('d', (j, q), half)
            expert_out(1, q, half)
            if q + 2 < groups:
                start('d', (j, q + 2), half)
            else:
                @pl.when(j + 1 < n_col)
                def _():
                    start('d', (j + 1, q + 2 - groups), half)

        @pl.when(j == 0)
        def _():
            for k in range(4):
                table_back(k).wait()

        to_sibling(1, j)
        to_peer(1, j)
        return carry

    def down_a_gate_b(t, carry):
        first = base_mix + t * (groups + each)
        for q in range(groups):
            half = half_at(first + q)
            wait('d', (t, q), half)
            expert_out(0, q, half)
            if q + 2 < groups:
                start('d', (t, q + 2), half)
            elif q + 2 == groups:
                start('g', t * each, half)
            else:
                @pl.when(t * each + 1 < n_first)
                def _():
                    start('g', t * each + 1, half)

                @pl.when(t * each + 1 >= n_first)
                def _():
                    start('d', (0, 0), half)
        to_sibling(0, t)

        @pl.when(t == n_col - 1)
        def _():
            table_back(1).start()
            table_back(3).start()

        @pl.when(t == 0)
        def _():
            for k in range(4):
                dispatch(1, k, 0, n_first, SLOTS, 0)

        to_peer(0, t)

        @pl.when(t == n_col - 1)
        def _():
            table_back(0).start()
            table_back(2).start()

        def hidden(r):
            half = half_at(first + groups + r)
            e = t * each + r
            ahead = r + lax.div(t + 1, n_col)
            wait('g', e, half)
            expert_hidden(
                e, half, SLOTS, (local_n,), lambda slots: start('d', (lax.rem(t + 1, n_col), ahead), half, slots))

        hidden(0)

        @pl.when(t * each + 1 < n_first)
        def _():
            hidden(1)

        return carry

    def forward(m):
        rows_out[2 * m].wait_recv()
        c = remote(xv.at[m, 2], xv.at[m, 3], row_send.at[m, 2], row_recv.at[m, 2], sib)
        c.start()
        return c

    for i in (n_q - 2, n_q - 1):
        qkv_out(i).wait()
    loads[2].wait()
    rows_out[1].wait_recv()
    dispatch(0, 0, 0, n_first, SLOTS, 0)
    dispatch(0, 1, 0, n_first, SLOTS, 0)
    forward_a = forward(0)
    dispatch(0, 2, 0, n_first, SLOTS, 0)
    forward_a.wait_recv()
    dispatch(0, 3, 0, n_first, SLOTS, 0)
    first_hidden()
    lax.fori_loop(1, n_first, gate_up_a, 0)
    for k in range(4):
        dispatch(0, k, n_first, n_both, 2 * SLOTS, 0)
    rows_out[3].wait_recv()
    dispatch(1, 0, n_first, n_both, 2 * SLOTS, SLOTS)
    dispatch(1, 1, n_first, n_both, 2 * SLOTS, SLOTS)
    forward_b = forward(1)
    dispatch(1, 2, n_first, n_both, 2 * SLOTS, SLOTS)
    forward_b.wait_recv()
    dispatch(1, 3, n_first, n_both, 2 * SLOTS, SLOTS)
    lax.fori_loop(0, n_both, gate_up_ab, 0)
    lax.fori_loop(0, n_col, down_a_gate_b, 0)
    lax.fori_loop(0, n_col, down_b, 0)

    sib_out(n_col - 1).wait_send()
    mine_out(1, n_col - 1).wait()
    outs = []
    for m in range(2):
        for j in range(n_col):
            slot = j % 2
            cols = slice(j * CHUNK, (j + 1) * CHUNK)
            back_out(m, j).wait_recv()
            parts = [
                pltpu.make_async_copy(mine_hbm.at[m, :, cols], zr.at[slot, 0], final_sem.at[0]),
                pltpu.make_async_copy(back_hbm.at[m, :, cols], zr.at[slot, 1], final_sem.at[1]),
            ]
            for c in parts:
                c.start()
            for c in parts:
                c.wait()
            total_row = xv[m, 0, :, cols].astype(F32) + (zr[slot, 0] + zr[slot, 1])
            xs[m * tok:(m + 1) * tok, cols] = total_row.astype(BF16)
            out = pltpu.make_async_copy(
                xs.at[m * tok:(m + 1) * tok, cols], (outa_hbm, outb_hbm)[m].at[:, cols], last_sem.at[m, j])
            out.start()
            outs.append(out)
    for j in (n_col - 2, n_col - 1):
        back_out(1, j).wait_send()
    for c in rows_out + [forward_a, forward_b]:
        c.wait_send()
    for c in outs:
        c.wait()


def moe_layer(x_a, h_b, attn_b, r_a, r_b, g_a, g_b, w_qkv, w_o, w_gate, w_up, w_down):
    tok, dim = x_a.shape
    local_n, ff, _ = w_down.shape
    hbm = pl.BlockSpec(memory_space=pl.ANY)
    dma = pltpu.SemaphoreType.DMA
    flops = 2 * tok * dim * (dim + w_qkv.shape[1]) + local_n * 2 * SLOTS * 6 * dim * ff
    return pl.pallas_call(
        layer_kernel,
        in_specs=[hbm] * 12,
        out_specs=[hbm] * 6,
        out_shape=[
            jax.ShapeDtypeStruct((2, tok, dim), F32),
            jax.ShapeDtypeStruct((2, tok, dim), F32),
            jax.ShapeDtypeStruct((tok, dim), BF16),
            jax.ShapeDtypeStruct((tok, dim), BF16),
            jax.ShapeDtypeStruct((tok, w_qkv.shape[1]), BF16),
            jax.ShapeDtypeStruct((4, 3, tok, local_n * WIN), BF16),
        ],
        scratch_shapes=[
            pltpu.VMEM((2, 4, tok, dim), BF16),
            pltpu.VMEM(((local_n + local_n % 2) * SLOTS, dim), BF16),
            pltpu.VMEM((2 * local_n * SLOTS, ff), BF16),
            pltpu.VMEM((2, dim, 5 * CHUNK + 256), BF16),
            pltpu.VMEM((4, 3, tok, local_n * WIN), BF16),
            pltpu.VMEM((4, 2, 4, tok), jnp.int32),
            pltpu.VMEM((4, 2, 4, tok), F32),
            pltpu.VMEM((2, 2, 4, 16, tok), F32),
            pltpu.VMEM((2, tok, CHUNK), F32),
            pltpu.VMEM((2, 2, tok, CHUNK), F32),
            pltpu.VMEM((2, tok, CHUNK), F32),
            pltpu.VMEM((tok, CHUNK), F32),
            dma((2, SET)), dma((2,)), dma((7,)), dma((2,)), dma((3, 4)), dma((3, 4)), dma((2, 3)), dma((2, 3)),
            dma(()), dma((2,)), dma((2,)), dma((2, dim // CHUNK)), dma(()), dma((2, dim // CHUNK)), dma((2,)), dma((4,)), dma((2,)),
        ],
        compiler_params=pltpu.CompilerParams(
            collective_id=0, has_side_effects=True, vmem_limit_bytes=VMEM_LIMIT),
        cost_estimate=pl.CostEstimate(flops=flops, bytes_accessed=local_n * 6 * dim * ff, transcendentals=0),
        name='moe_layer',
    )(x_a, h_b, attn_b, r_a, r_b, g_a, g_b, w_qkv, w_o, w_gate, w_up, w_down)


def hand_on_kernel(n, *refs):
    ins, outs, bufs = refs[:n], refs[n:2 * n], refs[2 * n:3 * n]
    in_sem, out_sem = refs[3 * n:]
    parts = []
    for a in range(n):
        for p in range(ins[a].shape[1] // 1024):
            parts.append((a, slice(1024 * p, 1024 * (p + 1)), len(parts)))
    gets = [pltpu.make_async_copy(ins[a].at[:, c], bufs[a].at[:, c], in_sem.at[i]) for a, c, i in parts]
    puts = [pltpu.make_async_copy(bufs[a].at[:, c], outs[a].at[:, c], out_sem.at[i]) for a, c, i in parts]
    for g in gets:
        g.start()
    for g, p in zip(gets, puts):
        g.wait()
        p.start()
    for p in puts:
        p.wait()


def hand_on(*arrays):
    n = len(arrays)
    count = sum(a.shape[1] // 1024 for a in arrays)
    hbm = pl.BlockSpec(memory_space=pl.ANY)
    return pl.pallas_call(
        functools.partial(hand_on_kernel, n),
        in_specs=[hbm] * n,
        out_specs=[hbm] * n,
        out_shape=[jax.ShapeDtypeStruct(a.shape, a.dtype) for a in arrays],
        scratch_shapes=[pltpu.VMEM(a.shape, a.dtype) for a in arrays] + [
            pltpu.SemaphoreType.DMA((count,)), pltpu.SemaphoreType.DMA((count,))],
        compiler_params=pltpu.CompilerParams(vmem_limit_bytes=VMEM_LIMIT),
        name='hand_on',
    )(*arrays)


def solution(mesh):
    def local_step(x_a, route_a, gate_a, h_b, attn_b, route_b, gate_b, w_qkv, w_o, w_gate, w_up, w_down):
        _, _, out_a, out_b, qkv_b, _ = moe_layer(
            x_a, h_b, attn_b, route_a.T, route_b.T, gate_a.T, gate_b.T, w_qkv, w_o, w_gate, w_up, w_down)
        out_a, out_b, qkv_b = hand_on(out_a, out_b, qkv_b)
        return out_a, out_b, qkv_b

    row_spec = P(('dp', 'ep'), None)
    full_spec = P(None, None)
    expert_spec = P('ep', None, None)
    return jax.shard_map(
        local_step,
        mesh=mesh,
        in_specs=(row_spec, row_spec, row_spec, row_spec, row_spec, row_spec, row_spec, full_spec, full_spec, expert_spec, expert_spec, expert_spec),
        out_specs=(row_spec, row_spec, row_spec),
        check_vma=False,
    )
```

```python
import functools

import jax
import jax.numpy as jnp
from jax import lax
from jax.experimental import pallas as pl
from jax.experimental.pallas import tpu as pltpu
from jax.sharding import PartitionSpec as P

F32 = jnp.float32
BF16 = jnp.bfloat16
CAP = 36
STRIDE = 32
WIN = 48
SLOTS = 144
CHUNK = 512
SET = 6
VMEM_LIMIT = 67043328


def dot(a, b):
    return jnp.dot(a, b, preferred_element_type=F32)


def layer_kernel(
    x_hbm, h_hbm, attn_hbm, ra_hbm, rb_hbm, ga_hbm, gb_hbm, wqkv_hbm, wo_hbm, wg_hbm, wu_hbm, wd_hbm,
    mine_hbm, back_hbm, outa_hbm, outb_hbm, qkv_hbm,
    xv, xs, hh, ring, gm, rv, gv, pt, zs, zr, xsend, mstage,
    ring_sem, tail_sem, load_sem, out_sem, meta_send, meta_recv, row_send, row_recv,
    zs_sem, zr_sem, xsend_sem, back_sem, mine_sem, last_sem, final_sem, early_sem,
):
    tok, dim = x_hbm.shape
    local_n, ff, _ = wd_hbm.shape
    n_first = local_n // 2
    n_both = local_n - n_first
    per = 5
    n_col = dim // CHUNK
    me = lax.axis_index('ep')
    sib = {'ep': me + 1 - 2 * lax.rem(me, 2)}
    peer = {'ep': lax.rem(me + 2, 4)}
    mesh_id = pl.DeviceIdType.MESH

    def remote(src, dst, send, recv, who):
        return pltpu.make_async_remote_copy(
            src_ref=src, dst_ref=dst, send_sem=send, recv_sem=recv, device_id=who, device_id_type=mesh_id)

    groups = local_n // per
    each = (n_first + n_col - 1) // n_col
    n_q = wqkv_hbm.shape[1] // (4 * CHUNK)
    base_g = 1 + n_q
    base_mix = base_g + local_n - 1
    base_db = base_mix + n_col * groups + n_first

    def half_at(it):
        return it % 2 if isinstance(it, int) else lax.rem(it, 2)

    def copies(kind, i, half, slots=range(SET)):
        out = []

        def add(src, slot, rows, lo, hi, sem):
            if slot in slots:
                out.append(pltpu.make_async_copy(src, ring.at[half, :rows, slot * CHUNK + lo:slot * CHUNK + hi], sem))

        if kind in ('o', 'q'):
            for c in range(4):
                src = wo_hbm if kind == 'o' else wqkv_hbm
                cols = pl.ds(pl.multiple_of((4 * i + c) * CHUNK, CHUNK), CHUNK)
                add(src.at[:, cols], c, dim, 0, CHUNK, ring_sem.at[half, c])
        elif kind == 'g':
            for p in range(2):
                cols = slice(p * CHUNK, (p + 1) * CHUNK)
                add(wg_hbm.at[i, :, cols], 2 * p, dim, 0, CHUNK, ring_sem.at[half, 2 * p])
                add(wu_hbm.at[i, :, cols], 2 * p + 1, dim, 0, CHUNK, ring_sem.at[half, 2 * p + 1])
            add(wg_hbm.at[i, :, 1024:1408], 4, dim, 0, 384, ring_sem.at[half, 4])
            add(wu_hbm.at[i, :, 1280:1408], 4, dim, 384, 512, tail_sem.at[half])
            add(wu_hbm.at[i, :, 1024:1280], 5, dim, 0, 256, ring_sem.at[half, 5])
        else:
            j, q = i
            cols = pl.ds(pl.multiple_of(j * CHUNK, CHUNK), CHUNK)
            for c in range(per):
                add(wd_hbm.at[q * per + c, :, cols], c, ff, 0, CHUNK, ring_sem.at[half, c])
        return out

    def start(*args):
        for c in copies(*args):
            c.start()

    def wait(*args):
        for c in copies(*args):
            c.wait()

    barrier = pltpu.get_barrier_semaphore()
    for who in (sib, peer):
        pl.semaphore_signal(barrier, inc=1, device_id=who, device_id_type=mesh_id)
    pl.semaphore_wait(barrier, 2)

    loads = [
        pltpu.make_async_copy(attn_hbm, xs.at[0:tok], load_sem.at[0]),
        pltpu.make_async_copy(h_hbm, xs.at[tok:2 * tok], load_sem.at[1]),
        pltpu.make_async_copy(x_hbm, xv.at[0, 0], load_sem.at[2]),
    ]
    meta = [(ra_hbm, rv, 0), (rb_hbm, rv, 1), (ga_hbm, gv, 0), (gb_hbm, gv, 1)]
    for i, (src, dst, m) in enumerate(meta):
        loads.append(pltpu.make_async_copy(src, dst.at[0, m], load_sem.at[3 + i]))
    for c in loads[:2]:
        c.start()
    start('o', 0, 0)
    meta_out = []
    for way, who, place in ((0, peer, 2), (1, sib, 1)):
        for i, (src, dst, m) in enumerate(meta):
            meta_out.append(remote(src, dst.at[place, m], meta_send.at[way, i], meta_recv.at[way, i], who))
    rows_out = [remote(x_hbm, xv.at[0, 2], row_send.at[0, 0], row_recv.at[0, 0], peer),
                remote(x_hbm, xv.at[0, 1], row_send.at[0, 1], row_recv.at[0, 1], sib)]
    for c in meta_out + rows_out:
        c.start()
    for c in loads[2:]:
        c.start()
    start('q', 0, 1)
    for c in loads[:2]:
        c.wait()

    wait('o', 0, 0)
    for c in range(4):
        cols = slice(c * CHUNK, (c + 1) * CHUNK)
        proj = dot(xs[0:tok, :], ring[0, :, cols]).astype(BF16)
        xv[1, 0, :, cols] = (xs[tok:2 * tok, cols].astype(F32) + proj.astype(F32)).astype(BF16)
    start('q', 1, 0)
    u_rows = [remote(xv.at[1, 0], xv.at[1, 2], row_send.at[1, 0], row_recv.at[1, 0], peer),
              remote(xv.at[1, 0], xv.at[1, 1], row_send.at[1, 1], row_recv.at[1, 1], sib)]
    rows_out += u_rows

    def qkv_out(i):
        rows = pl.ds(pl.multiple_of((2 + lax.rem(i, 2)) * tok, tok), tok)
        cols = pl.ds(pl.multiple_of(i * 4 * CHUNK, 4 * CHUNK), 4 * CHUNK)
        return pltpu.make_async_copy(xs.at[rows], qkv_hbm.at[:, cols], out_sem.at[lax.rem(i, 2)])

    def qkv_step(i, carry):
        half = half_at(1 + i)
        wait('q', i, half)

        @pl.when(i >= 2)
        def _():
            qkv_out(i - 2).wait()

        rows = pl.ds(pl.multiple_of((2 + lax.rem(i, 2)) * tok, tok), tok)
        for c in range(4):
            out = dot(xs[tok:2 * tok, :], ring[half, :, c * CHUNK:(c + 1) * CHUNK])
            xs[rows, c * CHUNK:(c + 1) * CHUNK] = out.astype(BF16)

        @pl.when(i + 2 < n_q)
        def _():
            start('q', i + 2, half)

        @pl.when(i + 2 >= n_q)
        def _():
            start('g', i + 3 - n_q, half)

        qkv_out(i).start()

        @pl.when(i == 0)
        def _():
            for c in u_rows:
                c.start()

        return carry

    lax.fori_loop(0, n_q, qkv_step, 0)
    early = [pltpu.make_async_copy(wg_hbm.at[0], hh.at[0:dim], early_sem.at[0]),
             pltpu.make_async_copy(wu_hbm.at[0], hh.at[dim:2 * dim], early_sem.at[1])]
    for c in early:
        c.start()

    for c in meta_out[:4]:
        c.wait_recv()
    for i, (_, dst, m) in enumerate(meta):
        meta_out.append(remote(dst.at[2, m], dst.at[3, m], meta_send.at[2, i], meta_recv.at[2, i], sib))
        meta_out[-1].start()
    for c in loads[3:]:
        c.wait()
    for c in meta_out[4:]:
        c.wait_recv()
    for c in meta_out:
        c.wait_send()
    first_expert = me * local_n
    expert_rows = lax.broadcasted_iota(jnp.int32, (16, tok), 0)
    before = (lax.broadcasted_iota(jnp.int32, (tok, tok), 0)
              < lax.broadcasted_iota(jnp.int32, (tok, tok), 1)).astype(F32).astype(BF16)
    for k in range(4):
        for m in range(2):
            hit = jnp.zeros((16, tok), F32)
            gate = jnp.zeros((16, tok), F32)
            for c in range(4):
                local = rv[k, m, c:c + 1, :] - first_expert
                same = jnp.broadcast_to(local, (16, tok)) == expert_rows
                hit = jnp.where(same, 1.0, hit)
                gate = jnp.where(same, jnp.broadcast_to(gv[k, m, c:c + 1, :], (16, tok)), gate)
            rank = dot(hit.astype(BF16), before)
            pt[0, m, k] = jnp.where(hit > 0.5, rank + 4.0 * k, -1.0)
            pt[1, m, k] = gate

    def mix_table(m, k):
        lanes = gm.shape[3]
        col = lax.broadcasted_iota(jnp.int32, (16, lanes), 1)
        first = WIN * lax.broadcasted_iota(jnp.int32, (16, lanes), 0)
        inside = (col >= first) & (col < first + WIN)
        expand = jnp.where(inside, 1.0, 0.0).astype(BF16)
        offset = jnp.sum(jnp.where(inside, (col - first).astype(F32), 0.0), axis=0, keepdims=True)
        here = dot(pt[0, m, k].T.astype(BF16), expand) == offset
        gate = pt[1, m, k].T
        for i in range(3):
            part = gate.astype(BF16)
            gate = gate - part.astype(F32)
            gm[k, i] = jnp.where(here, dot(part, expand), 0.0).astype(BF16)

    def dispatch(m, k, e0, ne, rows_per, shift):
        rows = lax.broadcasted_iota(jnp.int32, (WIN, tok), 0).astype(F32)
        pick = jnp.concatenate([
            jnp.where(jnp.broadcast_to(pt[0, m, k, e:e + 1, :], (WIN, tok)) == rows, 1.0, 0.0).astype(BF16)
            for e in range(e0, e0 + ne)], axis=0)
        for c in range(0, dim, CHUNK):
            got = dot(pick, xv[m, k, :, c:c + CHUNK]).astype(BF16)
            for e in range(ne):
                lo = e * rows_per + shift + STRIDE * k
                piece = got[e * WIN:(e + 1) * WIN]
                if k == 0:
                    xs[lo:lo + WIN, c:c + CHUNK] = piece
                else:
                    xs[lo:lo + 16, c:c + CHUNK] += piece[:16]
                    xs[lo + 16:lo + WIN, c:c + CHUNK] = piece[16:]

    def hidden_rows(i):
        return pl.ds(pl.multiple_of(i * SLOTS, 16), SLOTS)

    def first_hidden():
        for c in early:
            c.wait()
        x = slice(0, SLOTS)
        spare = slice(n_first * SLOTS, (n_first + 1) * SLOTS)
        for lo in range(0, ff, CHUNK):
            hi = min(lo + CHUNK, ff)
            g = dot(xs[x, :], hh[0:dim, lo:hi])
            u = dot(xs[x, :], hh[dim:2 * dim, lo:hi])
            xs[spare, lo:hi] = (jax.nn.silu(g) * u).astype(BF16)
        hh[0:SLOTS, :] = xs[spare, 0:ff]

    def expert_hidden(i, half, rows_per, where, refill):
        rows = pl.ds(pl.multiple_of(i * rows_per, 16), rows_per)

        def put(lo, hi, g, u):
            h = (jax.nn.silu(g) * u).astype(BF16)
            for r, shift in enumerate(where):
                hh[hidden_rows(i + shift), lo:hi] = h[r * SLOTS:(r + 1) * SLOTS]

        for p in range(2):
            g = dot(xs[rows, :], ring[half, :, 2 * p * CHUNK:(2 * p + 1) * CHUNK])
            u = dot(xs[rows, :], ring[half, :, (2 * p + 1) * CHUNK:(2 * p + 2) * CHUNK])
            put(p * CHUNK, (p + 1) * CHUNK, g, u)
            refill((2 * p, 2 * p + 1))
        t = dot(xs[rows, :], ring[half, :, 4 * CHUNK:5 * CHUNK])
        u = dot(xs[rows, :], ring[half, :, 5 * CHUNK:])
        put(1024, 1280, t[:, :256], u)
        put(1280, 1408, t[:, 256:384], t[:, 384:512])
        refill((4, 5))

    def gate_up_a(i, carry):
        half = half_at(base_g + i - 1)
        wait('g', i, half)
        expert_hidden(i, half, SLOTS, (0,), lambda slots: start('g', i + 2, half, slots))

        @pl.when(i <= 4)
        def _():
            mix_table(0, i - 1)

        return carry

    def gate_up_ab(i, carry):
        e = n_first + i
        half = half_at(base_g + e - 1)
        wait('g', e, half)

        def refill(slots):
            if slots[0] == 0:
                return
            ready = range(4) if slots[0] == 2 else range(4, SET)

            @pl.when(e + 2 < local_n)
            def _():
                start('g', e + 2, half, ready)

            @pl.when(e + 2 >= local_n)
            def _():
                start('d', (0, e + 2 - local_n), half, ready)

        expert_hidden(i, half, 2 * SLOTS, (n_first, local_n + n_first), refill)
        return carry

    def mine_out(m, j):
        cols = pl.ds(pl.multiple_of(j * CHUNK, CHUNK), CHUNK)
        return pltpu.make_async_copy(mstage, mine_hbm.at[m, :, cols], mine_sem)

    def back_out(m, j):
        slot = lax.rem(j, 2)
        cols = pl.ds(pl.multiple_of(j * CHUNK, CHUNK), CHUNK)
        return remote(xsend.at[slot], back_hbm.at[m, :, cols], xsend_sem.at[slot], back_sem.at[m, j], peer)

    def sib_out(j):
        slot = lax.rem(j, 2)
        return remote(zs, zr.at[slot], zs_sem, zr_sem.at[slot], sib)

    y_row = n_first * SLOTS
    y_per = local_n - n_first

    def expert_out(m, q, half):
        for c in range(per):
            e = q * per + c
            y = dot(hh[hidden_rows(e + m * local_n), :], ring[half, :ff, c * CHUNK:(c + 1) * CHUNK])
            rows = pl.ds(pl.multiple_of(y_row + lax.rem(e, y_per) * SLOTS, 16), SLOTS)
            cols = pl.ds(pl.multiple_of((e // y_per) * CHUNK, CHUNK), CHUNK)
            xs[rows, cols] = y.astype(BF16)

    def mix(k):
        pieces = []
        for e in range(local_n):
            lo = y_row + (e % y_per) * SLOTS + STRIDE * k
            c = (e // y_per) * CHUNK
            pieces.append(xs[lo:lo + WIN, c:c + CHUNK])
        y = jnp.concatenate(pieces, axis=0)
        return dot(gm[k, 0], y) + dot(gm[k, 1], y) + dot(gm[k, 2], y)

    def to_sibling(m, j):
        if m == 0:
            @pl.when(j >= 1)
            def _():
                sib_out(j - 1).wait_send()
        else:
            sib_out(j + 1).wait_send()
        zs[0] = mix(1)
        zs[1] = mix(3)
        sib_out(j).start()

    def to_peer(m, j):
        slot = lax.rem(j, 2)
        if m == 0:
            @pl.when(j >= 1)
            def _():
                mine_out(0, j - 1).wait()

            @pl.when(j >= 2)
            def _():
                back_out(0, j - 2).wait_send()
        else:
            mine_out(m, j).wait()
            back_out(m, j).wait_send()
        mstage[...] = mix(0)
        xsend[slot] = mix(2)
        sib_out(j).wait_recv()
        xsend[slot] = xsend[slot] + zr[slot, 1]
        back_out(m, j).start()
        mstage[...] = mstage[...] + zr[slot, 0]
        mine_out(m, j).start()

    def down_b(j, carry):
        for q in range(groups):
            half = half_at(base_db + j * groups + q)
            wait('d', (j, q), half)
            expert_out(1, q, half)
            if q + 2 < groups:
                start('d', (j, q + 2), half)
            else:
                @pl.when(j + 1 < n_col)
                def _():
                    start('d', (j + 1, q + 2 - groups), half)

        to_sibling(1, j)
        to_peer(1, j)
        return carry

    def down_a_gate_b(t, carry):
        first = base_mix + t * (groups + each)
        for q in range(groups):
            half = half_at(first + q)
            wait('d', (t, q), half)
            expert_out(0, q, half)
            if q + 2 < groups:
                start('d', (t, q + 2), half)
            elif q + 2 == groups:
                start('g', t * each, half)
            else:
                @pl.when(t * each + 1 < n_first)
                def _():
                    start('g', t * each + 1, half)

                @pl.when(t * each + 1 >= n_first)
                def _():
                    start('d', (0, 0), half)
        to_sibling(0, t)

        @pl.when(t == n_col - 1)
        def _():
            mix_table(1, 1)
            mix_table(1, 3)

        @pl.when(t == 0)
        def _():
            for k in range(4):
                dispatch(1, k, 0, n_first, SLOTS, 0)

        to_peer(0, t)

        @pl.when(t == n_col - 1)
        def _():
            mix_table(1, 0)
            mix_table(1, 2)

        def hidden(r):
            half = half_at(first + groups + r)
            e = t * each + r
            ahead = r + lax.div(t + 1, n_col)
            wait('g', e, half)
            expert_hidden(
                e, half, SLOTS, (local_n,), lambda slots: start('d', (lax.rem(t + 1, n_col), ahead), half, slots))

        hidden(0)

        @pl.when(t * each + 1 < n_first)
        def _():
            hidden(1)

        return carry

    def forward(m):
        rows_out[2 * m].wait_recv()
        c = remote(xv.at[m, 2], xv.at[m, 3], row_send.at[m, 2], row_recv.at[m, 2], sib)
        c.start()
        return c

    for i in (n_q - 2, n_q - 1):
        qkv_out(i).wait()
    loads[2].wait()
    rows_out[1].wait_recv()
    dispatch(0, 0, 0, n_first, SLOTS, 0)
    dispatch(0, 1, 0, n_first, SLOTS, 0)
    forward_a = forward(0)
    dispatch(0, 2, 0, n_first, SLOTS, 0)
    forward_a.wait_recv()
    dispatch(0, 3, 0, n_first, SLOTS, 0)
    first_hidden()
    lax.fori_loop(1, n_first, gate_up_a, 0)
    for k in range(4):
        dispatch(0, k, n_first, n_both, 2 * SLOTS, 0)
    rows_out[3].wait_recv()
    dispatch(1, 0, n_first, n_both, 2 * SLOTS, SLOTS)
    dispatch(1, 1, n_first, n_both, 2 * SLOTS, SLOTS)
    forward_b = forward(1)
    dispatch(1, 2, n_first, n_both, 2 * SLOTS, SLOTS)
    forward_b.wait_recv()
    dispatch(1, 3, n_first, n_both, 2 * SLOTS, SLOTS)
    lax.fori_loop(0, n_both, gate_up_ab, 0)
    lax.fori_loop(0, n_col, down_a_gate_b, 0)
    lax.fori_loop(0, n_col, down_b, 0)

    sib_out(n_col - 1).wait_send()
    mine_out(1, n_col - 1).wait()
    outs = []
    for m in range(2):
        for j in range(n_col):
            slot = j % 2
            cols = slice(j * CHUNK, (j + 1) * CHUNK)
            if (m, j) == (1, n_col - 1):
                out = pltpu.make_async_copy(xv.at[m, 0, :, cols], outb_hbm.at[:, cols], last_sem.at[m, j])
                out.start()
                outs.append(out)
                back_out(m, j).wait_recv()
                continue
            back_out(m, j).wait_recv()
            parts = [
                pltpu.make_async_copy(mine_hbm.at[m, :, cols], zr.at[slot, 0], final_sem.at[0]),
                pltpu.make_async_copy(back_hbm.at[m, :, cols], zr.at[slot, 1], final_sem.at[1]),
            ]
            for c in parts:
                c.start()
            for c in parts:
                c.wait()
            total_row = xv[m, 0, :, cols].astype(F32) + (zr[slot, 0] + zr[slot, 1])
            xs[m * tok:(m + 1) * tok, cols] = total_row.astype(BF16)
            out = pltpu.make_async_copy(
                xs.at[m * tok:(m + 1) * tok, cols], (outa_hbm, outb_hbm)[m].at[:, cols], last_sem.at[m, j])
            out.start()
            outs.append(out)
    for j in (n_col - 2, n_col - 1):
        back_out(1, j).wait_send()
    for c in rows_out + [forward_a, forward_b]:
        c.wait_send()
    for c in outs:
        c.wait()


def moe_layer(x_a, h_b, attn_b, r_a, r_b, g_a, g_b, w_qkv, w_o, w_gate, w_up, w_down):
    tok, dim = x_a.shape
    local_n, ff, _ = w_down.shape
    hbm = pl.BlockSpec(memory_space=pl.ANY)
    dma = pltpu.SemaphoreType.DMA
    flops = 2 * tok * dim * (dim + w_qkv.shape[1]) + local_n * 2 * SLOTS * 6 * dim * ff
    return pl.pallas_call(
        layer_kernel,
        in_specs=[hbm] * 12,
        out_specs=[hbm] * 5,
        out_shape=[
            jax.ShapeDtypeStruct((2, tok, dim), F32),
            jax.ShapeDtypeStruct((2, tok, dim), F32),
            jax.ShapeDtypeStruct((tok, dim), BF16),
            jax.ShapeDtypeStruct((tok, dim), BF16),
            jax.ShapeDtypeStruct((tok, w_qkv.shape[1]), BF16),
        ],
        scratch_shapes=[
            pltpu.VMEM((2, 4, tok, dim), BF16),
            pltpu.VMEM(((local_n + local_n % 2) * SLOTS, dim), BF16),
            pltpu.VMEM((2 * local_n * SLOTS, ff), BF16),
            pltpu.VMEM((2, dim, 5 * CHUNK + 256), BF16),
            pltpu.VMEM((4, 3, tok, local_n * WIN), BF16),
            pltpu.VMEM((4, 2, 4, tok), jnp.int32),
            pltpu.VMEM((4, 2, 4, tok), F32),
            pltpu.VMEM((2, 2, 4, 16, tok), F32),
            pltpu.VMEM((2, tok, CHUNK), F32),
            pltpu.VMEM((2, 2, tok, CHUNK), F32),
            pltpu.VMEM((2, tok, CHUNK), F32),
            pltpu.VMEM((tok, CHUNK), F32),
            dma((2, SET)), dma((2,)), dma((7,)), dma((2,)), dma((3, 4)), dma((3, 4)), dma((2, 3)), dma((2, 3)),
            dma(()), dma((2,)), dma((2,)), dma((2, dim // CHUNK)), dma(()), dma((2, dim // CHUNK)), dma((2,)), dma((2,)),
        ],
        compiler_params=pltpu.CompilerParams(
            collective_id=0, has_side_effects=True, vmem_limit_bytes=VMEM_LIMIT),
        cost_estimate=pl.CostEstimate(flops=flops, bytes_accessed=local_n * 6 * dim * ff, transcendentals=0),
        name='moe_layer',
    )(x_a, h_b, attn_b, r_a, r_b, g_a, g_b, w_qkv, w_o, w_gate, w_up, w_down)


def hand_on_kernel(mine, back, out_a, out_b, qkv, to_a, to_b, to_qkv, buf_a, buf_b, buf_qkv, sums, in_sem, out_sem, sum_sem):
    width = out_b.shape[1]
    last = slice(width - CHUNK, width)
    moves = [(out_b, buf_b, to_b, last)]
    for src, buf, dst in ((qkv, buf_qkv, to_qkv), (out_a, buf_a, to_a), (out_b, buf_b, to_b)):
        for lo in range(0, src.shape[1], 2 * CHUNK):
            hi = min(lo + 2 * CHUNK, src.shape[1] - (CHUNK if src is out_b else 0))
            moves.append((src, buf, dst, slice(lo, hi)))
    parts = [pltpu.make_async_copy(mine.at[1, :, last], sums.at[0], sum_sem.at[0]),
             pltpu.make_async_copy(back.at[1, :, last], sums.at[1], sum_sem.at[1])]
    gets = [pltpu.make_async_copy(s.at[:, c], b.at[:, c], in_sem.at[i]) for i, (s, b, _, c) in enumerate(moves)]
    puts = [pltpu.make_async_copy(b.at[:, c], d.at[:, c], out_sem.at[i]) for i, (_, b, d, c) in enumerate(moves)]
    for g in parts + gets:
        g.start()
    for i, (g, p) in enumerate(zip(gets, puts)):
        g.wait()
        if i == 0:
            for c in parts:
                c.wait()
            total = buf_b[:, last].astype(F32) + (sums[0] + sums[1])
            buf_b[:, last] = total.astype(BF16)
        p.start()
    for p in puts:
        p.wait()


def hand_on(mine, back, *arrays):
    tok = mine.shape[1]
    count = 1 + sum(a.shape[1] // (2 * CHUNK) for a in arrays)
    hbm = pl.BlockSpec(memory_space=pl.ANY)
    dma = pltpu.SemaphoreType.DMA
    return pl.pallas_call(
        hand_on_kernel,
        in_specs=[hbm] * 5,
        out_specs=[hbm] * 3,
        out_shape=[jax.ShapeDtypeStruct(a.shape, a.dtype) for a in arrays],
        scratch_shapes=[pltpu.VMEM(a.shape, a.dtype) for a in arrays] + [
            pltpu.VMEM((2, tok, CHUNK), F32), dma((count,)), dma((count,)), dma((2,))],
        compiler_params=pltpu.CompilerParams(vmem_limit_bytes=VMEM_LIMIT),
        name='hand_on',
    )(mine, back, *arrays)


def solution(mesh):
    def local_step(x_a, route_a, gate_a, h_b, attn_b, route_b, gate_b, w_qkv, w_o, w_gate, w_up, w_down):
        mine, back, out_a, out_b, qkv_b = moe_layer(
            x_a, h_b, attn_b, route_a.T, route_b.T, gate_a.T, gate_b.T, w_qkv, w_o, w_gate, w_up, w_down)
        out_a, out_b, qkv_b = hand_on(mine, back, out_a, out_b, qkv_b)
        return out_a, out_b, qkv_b

    row_spec = P(('dp', 'ep'), None)
    full_spec = P(None, None)
    expert_spec = P('ep', None, None)
    return jax.shard_map(
        local_step,
        mesh=mesh,
        in_specs=(row_spec, row_spec, row_spec, row_spec, row_spec, row_spec, row_spec, full_spec, full_spec, expert_spec, expert_spec, expert_spec),
        out_specs=(row_spec, row_spec, row_spec),
        check_vma=False,
    )
```

```python
import functools

import jax
import jax.numpy as jnp
from jax import lax
from jax.experimental import pallas as pl
from jax.experimental.pallas import tpu as pltpu
from jax.sharding import PartitionSpec as P

F32 = jnp.float32
BF16 = jnp.bfloat16
CAP = 36
STRIDE = 32
WIN = 48
SLOTS = 144
CHUNK = 512
SET = 6
VMEM_LIMIT = 67043328


def dot(a, b):
    return jnp.dot(a, b, preferred_element_type=F32)


def layer_kernel(
    x_hbm, h_hbm, attn_hbm, ra_hbm, rb_hbm, ga_hbm, gb_hbm, wqkv_hbm, wo_hbm, wg_hbm, wu_hbm, wd_hbm,
    mine_hbm, back_hbm, outa_hbm, outb_hbm, qkv_hbm,
    xv, xs, hh, ring, gm, rv, gv, pt, zs, zr, xsend, mstage,
    ring_sem, tail_sem, load_sem, out_sem, meta_send, meta_recv, row_send, row_recv,
    zs_sem, zr_sem, xsend_sem, back_sem, mine_sem, last_sem, final_sem, early_sem,
):
    tok, dim = x_hbm.shape
    local_n, ff, _ = wd_hbm.shape
    n_first = local_n // 2
    n_both = local_n - n_first
    per = 5
    n_col = dim // CHUNK
    me = lax.axis_index('ep')
    sib = {'ep': me + 1 - 2 * lax.rem(me, 2)}
    peer = {'ep': lax.rem(me + 2, 4)}
    mesh_id = pl.DeviceIdType.MESH

    def remote(src, dst, send, recv, who):
        return pltpu.make_async_remote_copy(
            src_ref=src, dst_ref=dst, send_sem=send, recv_sem=recv, device_id=who, device_id_type=mesh_id)

    groups = local_n // per
    each = (n_first + n_col - 1) // n_col
    n_q = wqkv_hbm.shape[1] // (4 * CHUNK)
    base_g = 1 + n_q
    base_mix = base_g + local_n - 1
    base_db = base_mix + n_col * groups + n_first

    def half_at(it):
        return it % 2 if isinstance(it, int) else lax.rem(it, 2)

    def copies(kind, i, half, slots=range(SET)):
        out = []

        def add(src, slot, rows, lo, hi, sem):
            if slot in slots:
                out.append(pltpu.make_async_copy(src, ring.at[half, :rows, slot * CHUNK + lo:slot * CHUNK + hi], sem))

        if kind in ('o', 'q'):
            for c in range(4):
                src = wo_hbm if kind == 'o' else wqkv_hbm
                cols = pl.ds(pl.multiple_of((4 * i + c) * CHUNK, CHUNK), CHUNK)
                add(src.at[:, cols], c, dim, 0, CHUNK, ring_sem.at[half, c])
        elif kind == 'g':
            for p in range(2):
                cols = slice(p * CHUNK, (p + 1) * CHUNK)
                add(wg_hbm.at[i, :, cols], 2 * p, dim, 0, CHUNK, ring_sem.at[half, 2 * p])
                add(wu_hbm.at[i, :, cols], 2 * p + 1, dim, 0, CHUNK, ring_sem.at[half, 2 * p + 1])
            add(wg_hbm.at[i, :, 1024:1408], 4, dim, 0, 384, ring_sem.at[half, 4])
            add(wu_hbm.at[i, :, 1280:1408], 4, dim, 384, 512, tail_sem.at[half])
            add(wu_hbm.at[i, :, 1024:1280], 5, dim, 0, 256, ring_sem.at[half, 5])
        else:
            j, q = i
            cols = pl.ds(pl.multiple_of(j * CHUNK, CHUNK), CHUNK)
            for c in range(per):
                add(wd_hbm.at[q * per + c, :, cols], c, ff, 0, CHUNK, ring_sem.at[half, c])
        return out

    def start(*args):
        for c in copies(*args):
            c.start()

    def wait(*args):
        for c in copies(*args):
            c.wait()

    barrier = pltpu.get_barrier_semaphore()
    for who in (sib, peer):
        pl.semaphore_signal(barrier, inc=1, device_id=who, device_id_type=mesh_id)
    pl.semaphore_wait(barrier, 2)

    loads = [
        pltpu.make_async_copy(attn_hbm, xs.at[0:tok], load_sem.at[0]),
        pltpu.make_async_copy(h_hbm, xs.at[tok:2 * tok], load_sem.at[1]),
        pltpu.make_async_copy(x_hbm, xv.at[0, 0], load_sem.at[2]),
    ]
    meta = [(ra_hbm, rv, 0), (rb_hbm, rv, 1), (ga_hbm, gv, 0), (gb_hbm, gv, 1)]
    for i, (src, dst, m) in enumerate(meta):
        loads.append(pltpu.make_async_copy(src, dst.at[0, m], load_sem.at[3 + i]))
    meta_out = []
    for way, who, place in ((0, peer, 2), (1, sib, 1)):
        for i, (src, dst, m) in enumerate(meta):
            meta_out.append(remote(src, dst.at[place, m], meta_send.at[way, i], meta_recv.at[way, i], who))
    rows_out = [remote(x_hbm, xv.at[0, 2], row_send.at[0, 0], row_recv.at[0, 0], peer),
                remote(x_hbm, xv.at[0, 1], row_send.at[0, 1], row_recv.at[0, 1], sib)]
    for c in meta_out + rows_out:
        c.start()
    for c in loads[:2]:
        c.start()
    start('o', 0, 0)
    for c in loads[2:]:
        c.start()
    start('q', 0, 1)
    for c in loads[:2]:
        c.wait()

    wait('o', 0, 0)
    for c in range(4):
        cols = slice(c * CHUNK, (c + 1) * CHUNK)
        proj = dot(xs[0:tok, :], ring[0, :, cols]).astype(BF16)
        xv[1, 0, :, cols] = (xs[tok:2 * tok, cols].astype(F32) + proj.astype(F32)).astype(BF16)
    start('q', 1, 0)
    u_rows = [remote(xv.at[1, 0], xv.at[1, 2], row_send.at[1, 0], row_recv.at[1, 0], peer),
              remote(xv.at[1, 0], xv.at[1, 1], row_send.at[1, 1], row_recv.at[1, 1], sib)]
    rows_out += u_rows

    def qkv_out(i):
        rows = pl.ds(pl.multiple_of((2 + lax.rem(i, 2)) * tok, tok), tok)
        cols = pl.ds(pl.multiple_of(i * 4 * CHUNK, 4 * CHUNK), 4 * CHUNK)
        return pltpu.make_async_copy(xs.at[rows], qkv_hbm.at[:, cols], out_sem.at[lax.rem(i, 2)])

    def qkv_step(i, carry):
        half = half_at(1 + i)
        wait('q', i, half)

        @pl.when(i >= 2)
        def _():
            qkv_out(i - 2).wait()

        rows = pl.ds(pl.multiple_of((2 + lax.rem(i, 2)) * tok, tok), tok)
        for c in range(4):
            out = dot(xs[tok:2 * tok, :], ring[half, :, c * CHUNK:(c + 1) * CHUNK])
            xs[rows, c * CHUNK:(c + 1) * CHUNK] = out.astype(BF16)

        @pl.when(i + 2 < n_q)
        def _():
            start('q', i + 2, half)

        @pl.when(i + 2 >= n_q)
        def _():
            start('g', i + 3 - n_q, half)

        qkv_out(i).start()

        @pl.when(i == 0)
        def _():
            for c in u_rows:
                c.start()

        return carry

    lax.fori_loop(0, n_q, qkv_step, 0)
    early = [pltpu.make_async_copy(wg_hbm.at[0], hh.at[0:dim], early_sem.at[0]),
             pltpu.make_async_copy(wu_hbm.at[0], hh.at[dim:2 * dim], early_sem.at[1])]
    for c in early:
        c.start()

    for c in meta_out[:4]:
        c.wait_recv()
    for i, (_, dst, m) in enumerate(meta):
        meta_out.append(remote(dst.at[2, m], dst.at[3, m], meta_send.at[2, i], meta_recv.at[2, i], sib))
        meta_out[-1].start()
    for c in loads[3:]:
        c.wait()
    for c in meta_out[4:]:
        c.wait_recv()
    for c in meta_out:
        c.wait_send()
    first_expert = me * local_n
    expert_rows = lax.broadcasted_iota(jnp.int32, (16, tok), 0)
    before = (lax.broadcasted_iota(jnp.int32, (tok, tok), 0)
              < lax.broadcasted_iota(jnp.int32, (tok, tok), 1)).astype(F32).astype(BF16)
    for k in range(4):
        for m in range(2):
            hit = jnp.zeros((16, tok), F32)
            gate = jnp.zeros((16, tok), F32)
            for c in range(4):
                local = rv[k, m, c:c + 1, :] - first_expert
                same = jnp.broadcast_to(local, (16, tok)) == expert_rows
                hit = jnp.where(same, 1.0, hit)
                gate = jnp.where(same, jnp.broadcast_to(gv[k, m, c:c + 1, :], (16, tok)), gate)
            rank = dot(hit.astype(BF16), before)
            pt[0, m, k] = jnp.where(hit > 0.5, rank + 4.0 * k, -1.0)
            pt[1, m, k] = gate

    def mix_table(m, k):
        lanes = gm.shape[3]
        col = lax.broadcasted_iota(jnp.int32, (16, lanes), 1)
        first = WIN * lax.broadcasted_iota(jnp.int32, (16, lanes), 0)
        inside = (col >= first) & (col < first + WIN)
        expand = jnp.where(inside, 1.0, 0.0).astype(BF16)
        offset = jnp.sum(jnp.where(inside, (col - first).astype(F32), 0.0), axis=0, keepdims=True)
        here = dot(pt[0, m, k].T.astype(BF16), expand) == offset
        gate = pt[1, m, k].T
        for i in range(3):
            part = gate.astype(BF16)
            gate = gate - part.astype(F32)
            gm[k, i] = jnp.where(here, dot(part, expand), 0.0).astype(BF16)

    def dispatch(m, k, e0, ne, rows_per, shift):
        rows = lax.broadcasted_iota(jnp.int32, (WIN, tok), 0).astype(F32)
        pick = jnp.concatenate([
            jnp.where(jnp.broadcast_to(pt[0, m, k, e:e + 1, :], (WIN, tok)) == rows, 1.0, 0.0).astype(BF16)
            for e in range(e0, e0 + ne)], axis=0)
        for c in range(0, dim, CHUNK):
            got = dot(pick, xv[m, k, :, c:c + CHUNK]).astype(BF16)
            for e in range(ne):
                lo = e * rows_per + shift + STRIDE * k
                piece = got[e * WIN:(e + 1) * WIN]
                if k == 0:
                    xs[lo:lo + WIN, c:c + CHUNK] = piece
                else:
                    xs[lo:lo + 16, c:c + CHUNK] += piece[:16]
                    xs[lo + 16:lo + WIN, c:c + CHUNK] = piece[16:]

    def hidden_rows(i):
        return pl.ds(pl.multiple_of(i * SLOTS, 16), SLOTS)

    def first_hidden():
        for c in early:
            c.wait()
        x = slice(0, SLOTS)
        spare = slice(n_first * SLOTS, (n_first + 1) * SLOTS)
        for lo in range(0, ff, CHUNK):
            hi = min(lo + CHUNK, ff)
            g = dot(xs[x, :], hh[0:dim, lo:hi])
            u = dot(xs[x, :], hh[dim:2 * dim, lo:hi])
            xs[spare, lo:hi] = (jax.nn.silu(g) * u).astype(BF16)
        hh[0:SLOTS, :] = xs[spare, 0:ff]

    def expert_hidden(i, half, rows_per, where, refill):
        rows = pl.ds(pl.multiple_of(i * rows_per, 16), rows_per)

        def put(lo, hi, g, u):
            h = (jax.nn.silu(g) * u).astype(BF16)
            for r, shift in enumerate(where):
                hh[hidden_rows(i + shift), lo:hi] = h[r * SLOTS:(r + 1) * SLOTS]

        for p in range(2):
            g = dot(xs[rows, :], ring[half, :, 2 * p * CHUNK:(2 * p + 1) * CHUNK])
            u = dot(xs[rows, :], ring[half, :, (2 * p + 1) * CHUNK:(2 * p + 2) * CHUNK])
            put(p * CHUNK, (p + 1) * CHUNK, g, u)
            refill((2 * p, 2 * p + 1))
        t = dot(xs[rows, :], ring[half, :, 4 * CHUNK:5 * CHUNK])
        u = dot(xs[rows, :], ring[half, :, 5 * CHUNK:])
        put(1024, 1280, t[:, :256], u)
        put(1280, 1408, t[:, 256:384], t[:, 384:512])
        refill((4, 5))

    def gate_up_a(i, carry):
        half = half_at(base_g + i - 1)
        wait('g', i, half)
        expert_hidden(i, half, SLOTS, (0,), lambda slots: start('g', i + 2, half, slots))

        @pl.when(i <= 4)
        def _():
            mix_table(0, i - 1)

        return carry

    def gate_up_ab(i, carry):
        e = n_first + i
        half = half_at(base_g + e - 1)
        wait('g', e, half)

        def refill(slots):
            if slots[0] == 0:
                return
            ready = range(4) if slots[0] == 2 else range(4, SET)

            @pl.when(e + 2 < local_n)
            def _():
                start('g', e + 2, half, ready)

            @pl.when(e + 2 >= local_n)
            def _():
                start('d', (0, e + 2 - local_n), half, ready)

        expert_hidden(i, half, 2 * SLOTS, (n_first, local_n + n_first), refill)
        return carry

    def mine_out(m, j):
        cols = pl.ds(pl.multiple_of(j * CHUNK, CHUNK), CHUNK)
        return pltpu.make_async_copy(mstage, mine_hbm.at[m, :, cols], mine_sem)

    def back_out(m, j):
        slot = lax.rem(j, 2)
        cols = pl.ds(pl.multiple_of(j * CHUNK, CHUNK), CHUNK)
        return remote(xsend.at[slot], back_hbm.at[m, :, cols], xsend_sem.at[slot], back_sem.at[m, j], peer)

    def sib_out(j):
        slot = lax.rem(j, 2)
        return remote(zs, zr.at[slot], zs_sem, zr_sem.at[slot], sib)

    y_row = n_first * SLOTS
    y_per = local_n - n_first

    def expert_out(m, q, half):
        for c in range(per):
            e = q * per + c
            y = dot(hh[hidden_rows(e + m * local_n), :], ring[half, :ff, c * CHUNK:(c + 1) * CHUNK])
            rows = pl.ds(pl.multiple_of(y_row + lax.rem(e, y_per) * SLOTS, 16), SLOTS)
            cols = pl.ds(pl.multiple_of((e // y_per) * CHUNK, CHUNK), CHUNK)
            xs[rows, cols] = y.astype(BF16)

    def mix(k):
        pieces = []
        for e in range(local_n):
            lo = y_row + (e % y_per) * SLOTS + STRIDE * k
            c = (e // y_per) * CHUNK
            pieces.append(xs[lo:lo + WIN, c:c + CHUNK])
        y = jnp.concatenate(pieces, axis=0)
        return dot(gm[k, 0], y) + dot(gm[k, 1], y) + dot(gm[k, 2], y)

    def to_sibling(m, j):
        if m == 0:
            @pl.when(j >= 1)
            def _():
                sib_out(j - 1).wait_send()
        else:
            sib_out(j + 1).wait_send()
        zs[0] = mix(1)
        zs[1] = mix(3)
        sib_out(j).start()

    def to_peer(m, j):
        slot = lax.rem(j, 2)
        if m == 0:
            @pl.when(j >= 1)
            def _():
                mine_out(0, j - 1).wait()

            @pl.when(j >= 2)
            def _():
                back_out(0, j - 2).wait_send()
        else:
            mine_out(m, j).wait()
            back_out(m, j).wait_send()
        mstage[...] = mix(0)
        xsend[slot] = mix(2)
        sib_out(j).wait_recv()
        xsend[slot] = xsend[slot] + zr[slot, 1]
        back_out(m, j).start()
        mstage[...] = mstage[...] + zr[slot, 0]
        mine_out(m, j).start()

    def down_b(j, carry):
        for q in range(groups):
            half = half_at(base_db + j * groups + q)
            wait('d', (j, q), half)
            expert_out(1, q, half)
            if q + 2 < groups:
                start('d', (j, q + 2), half)
            else:
                @pl.when(j + 1 < n_col)
                def _():
                    start('d', (j + 1, q + 2 - groups), half)

        to_sibling(1, j)
        to_peer(1, j)
        return carry

    def down_a_gate_b(t, carry):
        first = base_mix + t * (groups + each)
        for q in range(groups):
            half = half_at(first + q)
            wait('d', (t, q), half)
            expert_out(0, q, half)
            if q + 2 < groups:
                start('d', (t, q + 2), half)
            elif q + 2 == groups:
                start('g', t * each, half)
            else:
                @pl.when(t * each + 1 < n_first)
                def _():
                    start('g', t * each + 1, half)

                @pl.when(t * each + 1 >= n_first)
                def _():
                    start('d', (0, 0), half)
        to_sibling(0, t)

        @pl.when(t == n_col - 1)
        def _():
            mix_table(1, 1)
            mix_table(1, 3)

        @pl.when(t == 0)
        def _():
            for k in range(4):
                dispatch(1, k, 0, n_first, SLOTS, 0)

        to_peer(0, t)

        @pl.when(t == n_col - 1)
        def _():
            mix_table(1, 0)
            mix_table(1, 2)

        def hidden(r):
            half = half_at(first + groups + r)
            e = t * each + r
            ahead = r + lax.div(t + 1, n_col)
            wait('g', e, half)
            expert_hidden(
                e, half, SLOTS, (local_n,), lambda slots: start('d', (lax.rem(t + 1, n_col), ahead), half, slots))

        hidden(0)

        @pl.when(t * each + 1 < n_first)
        def _():
            hidden(1)

        return carry

    def forward(m):
        rows_out[2 * m].wait_recv()
        c = remote(xv.at[m, 2], xv.at[m, 3], row_send.at[m, 2], row_recv.at[m, 2], sib)
        c.start()
        return c

    for i in (n_q - 2, n_q - 1):
        qkv_out(i).wait()
    loads[2].wait()
    rows_out[1].wait_recv()
    dispatch(0, 0, 0, n_first, SLOTS, 0)
    dispatch(0, 1, 0, n_first, SLOTS, 0)
    forward_a = forward(0)
    dispatch(0, 2, 0, n_first, SLOTS, 0)
    forward_a.wait_recv()
    dispatch(0, 3, 0, n_first, SLOTS, 0)
    first_hidden()
    lax.fori_loop(1, n_first, gate_up_a, 0)
    dispatch(0, 0, n_first, n_both, 2 * SLOTS, 0)
    forward_b = forward(1)
    for k in range(1, 4):
        dispatch(0, k, n_first, n_both, 2 * SLOTS, 0)
    rows_out[3].wait_recv()
    for k in range(3):
        dispatch(1, k, n_first, n_both, 2 * SLOTS, SLOTS)
    forward_b.wait_recv()
    dispatch(1, 3, n_first, n_both, 2 * SLOTS, SLOTS)
    lax.fori_loop(0, n_both, gate_up_ab, 0)
    lax.fori_loop(0, n_col, down_a_gate_b, 0)
    lax.fori_loop(0, n_col, down_b, 0)

    sib_out(n_col - 1).wait_send()
    mine_out(1, n_col - 1).wait()
    outs = []
    for m in range(2):
        for j in range(n_col):
            slot = j % 2
            cols = slice(j * CHUNK, (j + 1) * CHUNK)
            if (m, j) == (1, n_col - 1):
                out = pltpu.make_async_copy(xv.at[m, 0, :, cols], outb_hbm.at[:, cols], last_sem.at[m, j])
                out.start()
                outs.append(out)
                back_out(m, j).wait_recv()
                continue
            back_out(m, j).wait_recv()
            parts = [
                pltpu.make_async_copy(mine_hbm.at[m, :, cols], zr.at[slot, 0], final_sem.at[0]),
                pltpu.make_async_copy(back_hbm.at[m, :, cols], zr.at[slot, 1], final_sem.at[1]),
            ]
            for c in parts:
                c.start()
            for c in parts:
                c.wait()
            total_row = xv[m, 0, :, cols].astype(F32) + (zr[slot, 0] + zr[slot, 1])
            xs[m * tok:(m + 1) * tok, cols] = total_row.astype(BF16)
            out = pltpu.make_async_copy(
                xs.at[m * tok:(m + 1) * tok, cols], (outa_hbm, outb_hbm)[m].at[:, cols], last_sem.at[m, j])
            out.start()
            outs.append(out)
    for j in (n_col - 2, n_col - 1):
        back_out(1, j).wait_send()
    for c in rows_out + [forward_a, forward_b]:
        c.wait_send()
    for c in outs:
        c.wait()


def moe_layer(x_a, h_b, attn_b, r_a, r_b, g_a, g_b, w_qkv, w_o, w_gate, w_up, w_down):
    tok, dim = x_a.shape
    local_n, ff, _ = w_down.shape
    hbm = pl.BlockSpec(memory_space=pl.ANY)
    dma = pltpu.SemaphoreType.DMA
    flops = 2 * tok * dim * (dim + w_qkv.shape[1]) + local_n * 2 * SLOTS * 6 * dim * ff
    return pl.pallas_call(
        layer_kernel,
        in_specs=[hbm] * 12,
        out_specs=[hbm] * 5,
        out_shape=[
            jax.ShapeDtypeStruct((2, tok, dim), F32),
            jax.ShapeDtypeStruct((2, tok, dim), F32),
            jax.ShapeDtypeStruct((tok, dim), BF16),
            jax.ShapeDtypeStruct((tok, dim), BF16),
            jax.ShapeDtypeStruct((tok, w_qkv.shape[1]), BF16),
        ],
        scratch_shapes=[
            pltpu.VMEM((2, 4, tok, dim), BF16),
            pltpu.VMEM(((local_n + local_n % 2) * SLOTS, dim), BF16),
            pltpu.VMEM((2 * local_n * SLOTS, ff), BF16),
            pltpu.VMEM((2, dim, 5 * CHUNK + 256), BF16),
            pltpu.VMEM((4, 3, tok, local_n * WIN), BF16),
            pltpu.VMEM((4, 2, 4, tok), jnp.int32),
            pltpu.VMEM((4, 2, 4, tok), F32),
            pltpu.VMEM((2, 2, 4, 16, tok), F32),
            pltpu.VMEM((2, tok, CHUNK), F32),
            pltpu.VMEM((2, 2, tok, CHUNK), F32),
            pltpu.VMEM((2, tok, CHUNK), F32),
            pltpu.VMEM((tok, CHUNK), F32),
            dma((2, SET)), dma((2,)), dma((7,)), dma((2,)), dma((3, 4)), dma((3, 4)), dma((2, 3)), dma((2, 3)),
            dma(()), dma((2,)), dma((2,)), dma((2, dim // CHUNK)), dma(()), dma((2, dim // CHUNK)), dma((2,)), dma((2,)),
        ],
        compiler_params=pltpu.CompilerParams(
            collective_id=0, has_side_effects=True, vmem_limit_bytes=VMEM_LIMIT),
        cost_estimate=pl.CostEstimate(flops=flops, bytes_accessed=local_n * 6 * dim * ff, transcendentals=0),
        name='moe_layer',
    )(x_a, h_b, attn_b, r_a, r_b, g_a, g_b, w_qkv, w_o, w_gate, w_up, w_down)


def hand_on_kernel(mine, back, out_a, out_b, qkv, to_a, to_b, to_qkv, buf_a, buf_b, buf_qkv, sums, in_sem, out_sem, sum_sem):
    width = out_b.shape[1]
    last = slice(width - CHUNK, width)
    moves = [(out_b, buf_b, to_b, last)]
    for src, buf, dst in ((qkv, buf_qkv, to_qkv), (out_a, buf_a, to_a), (out_b, buf_b, to_b)):
        for lo in range(0, src.shape[1], 2 * CHUNK):
            hi = min(lo + 2 * CHUNK, src.shape[1] - (CHUNK if src is out_b else 0))
            moves.append((src, buf, dst, slice(lo, hi)))
    parts = [pltpu.make_async_copy(mine.at[1, :, last], sums.at[0], sum_sem.at[0]),
             pltpu.make_async_copy(back.at[1, :, last], sums.at[1], sum_sem.at[1])]
    gets = [pltpu.make_async_copy(s.at[:, c], b.at[:, c], in_sem.at[i]) for i, (s, b, _, c) in enumerate(moves)]
    puts = [pltpu.make_async_copy(b.at[:, c], d.at[:, c], out_sem.at[i]) for i, (_, b, d, c) in enumerate(moves)]
    for g in parts + gets:
        g.start()
    for i, (g, p) in enumerate(zip(gets, puts)):
        g.wait()
        if i == 0:
            for c in parts:
                c.wait()
            total = buf_b[:, last].astype(F32) + (sums[0] + sums[1])
            buf_b[:, last] = total.astype(BF16)
        p.start()
    for p in puts:
        p.wait()


def hand_on(mine, back, *arrays):
    tok = mine.shape[1]
    count = 1 + sum(a.shape[1] // (2 * CHUNK) for a in arrays)
    hbm = pl.BlockSpec(memory_space=pl.ANY)
    dma = pltpu.SemaphoreType.DMA
    return pl.pallas_call(
        hand_on_kernel,
        in_specs=[hbm] * 5,
        out_specs=[hbm] * 3,
        out_shape=[jax.ShapeDtypeStruct(a.shape, a.dtype) for a in arrays],
        scratch_shapes=[pltpu.VMEM(a.shape, a.dtype) for a in arrays] + [
            pltpu.VMEM((2, tok, CHUNK), F32), dma((count,)), dma((count,)), dma((2,))],
        compiler_params=pltpu.CompilerParams(vmem_limit_bytes=VMEM_LIMIT),
        name='hand_on',
    )(mine, back, *arrays)


def solution(mesh):
    def local_step(x_a, route_a, gate_a, h_b, attn_b, route_b, gate_b, w_qkv, w_o, w_gate, w_up, w_down):
        mine, back, out_a, out_b, qkv_b = moe_layer(
            x_a, h_b, attn_b, route_a.T, route_b.T, gate_a.T, gate_b.T, w_qkv, w_o, w_gate, w_up, w_down)
        out_a, out_b, qkv_b = hand_on(mine, back, out_a, out_b, qkv_b)
        return out_a, out_b, qkv_b

    row_spec = P(('dp', 'ep'), None)
    full_spec = P(None, None)
    expert_spec = P('ep', None, None)
    return jax.shard_map(
        local_step,
        mesh=mesh,
        in_specs=(row_spec, row_spec, row_spec, row_spec, row_spec, row_spec, row_spec, full_spec, full_spec, expert_spec, expert_spec, expert_spec),
        out_specs=(row_spec, row_spec, row_spec),
        check_vma=False,
    )
```
